32 devices in a mesh: vel: 8 (over z, x), space: 4 (over y, core).
Axes of the slice: x: 2, y: 2, z: 4, core: 2. Of those that a mesh axis runs over, the one named last changes fastest.
Arguments:
- distribution: float32 [16384, 16, 256], P('vel', 'space'), may hold values from 0 to 5, as said below
- block_map: int32 [128], P('vel'), may hold values from 0 to 127, as said below
- inflow_mask: int32 [16, 256], P('space'), may hold values 0 or 1
- owner_map: int32 [8], replicated, may hold values from 0 to 7, each once
- inflow_scalars: float32 [2], replicated, may hold values from 0.8 to 1.25
- inflow_drift: float32 [3], replicated, may hold values from -0.3 to 0.3
Outputs:
- new_distribution: float32 [16384, 16, 256], P('vel', 'space')
- macro_fields: float32 [5, 4096], P(None, ('space', 'vel'))
The draws below stay inside these ranges and needn't reach their ends.
Inputs may be any that keep to these rules, and one draw needn't show every extreme that they name: `block_map`: a permutation of the velocity blocks. `owner_map`: a permutation of the owner positions. `distribution`: every entry is positive.
All inputs are finite; a program needn't handle non-finite values. No bound on the sum of `inflow_mask` on one device may be relied on, other than what follows from the above.
Results may differ from the reference program's by a relative error of at most 0.0001.
Values sent between devices are 32-bit elements; how exact they have to be, the bound alone decides.
No kernel may reach another device: no remote copies, remote signals or barrier semaphores. Data moves between devices by JAX's collectives and lax.ppermute only.
A program may use at most 192 MiB of HBM per device.

```python
import math
import jax
import jax.numpy as jnp
from jax import lax

NVX = 32
NVY = 32
NVZ = 16
V = 16384
VB = 128
NB = 128
NY = 16
NZ = 16
ITERS = 1
MSTEPS = 4
NXC = 16
OB = 128
N_VEL = 8
N_SPACE = 4


def velocity_order(key):
    return jax.random.permutation(jax.random.fold_in(key, 7), NB).astype(jnp.int32)


def draw_block_map(key, part):
    return velocity_order(key)


def draw_distribution(key, part):
    order = velocity_order(key)
    node_ids = (order[:, None] * VB + jnp.arange(VB, dtype=jnp.int32)[None, :]).reshape(-1)
    along_x = node_ids // (NVY * NVZ)
    along_y = node_ids // NVZ % NVY
    along_z = node_ids % NVZ
    speed_x = -3.5 + (along_x.astype(jnp.float32) + 0.5) * (7.0 / NVX)
    speed_y = -3.5 + (along_y.astype(jnp.float32) + 0.5) * (7.0 / NVY)
    speed_z = -3.5 + (along_z.astype(jnp.float32) + 0.5) * (7.0 / NVZ)
    cells = NXC * NY * NZ
    keys = jax.random.split(jax.random.fold_in(key, 19), 4)
    density = jnp.exp(jax.random.uniform(keys[0], (cells,), jnp.float32, math.log(0.6), math.log(1.6)))
    temper = jnp.exp(jax.random.uniform(keys[1], (cells,), jnp.float32, math.log(0.7), math.log(1.4)))
    drift = jax.random.uniform(keys[2], (3, cells), jnp.float32, -0.3, 0.3)
    noise = jax.random.uniform(keys[3], (V, cells), jnp.float32, 0.7, 1.3)
    rel_sq = (speed_x[:, None] - drift[0][None]) ** 2 + (speed_y[:, None] - drift[1][None]) ** 2 + (speed_z[:, None] - drift[2][None]) ** 2
    values = density[None] * temper[None] ** (-1.5) * jnp.exp(-rel_sq / (2.0 * temper[None])) * noise
    return values.reshape(V, NXC, NY * NZ).astype(jnp.float32)


def set_ends(values, key, smallest, high):
    extent = values.shape
    spot = [jax.random.randint(jax.random.fold_in(key, axis), (), 0, extent[axis]) for axis in range(len(extent))]
    values = values.at[tuple(spot)].set(smallest)
    longest = extent.index(max(extent))
    spot[longest] = (spot[longest] + 1) % extent[longest]
    return values.at[tuple(spot)].set(high)


def setup_inputs(seed: int = 0) -> dict:
    arg_keys = jax.random.split(jax.random.key(seed), 7)
    return {
        "distribution": draw_distribution(jax.random.fold_in(arg_keys[6], 71), 0),
        "block_map": draw_block_map(jax.random.fold_in(arg_keys[6], 71), 0),
        "inflow_mask": set_ends((jax.random.randint(arg_keys[2], (NXC, NY * NZ), 0, 16) < 1).astype(jnp.int32), jax.random.fold_in(arg_keys[2], 1), 0, 1),
        "owner_map": jax.random.permutation(arg_keys[3], N_VEL).astype(jnp.int32),
        "inflow_scalars": jnp.clip(jax.random.uniform(arg_keys[4], (2,), jnp.float32, 0.8, 1.25), 0.8, 1.25),
        "inflow_drift": jnp.clip(jax.random.uniform(arg_keys[5], (3,), jnp.float32, -0.3, 0.3), -0.3, 0.3),
    }


SPEED_LIMIT = 3.5
PRANDTL = 2.0 / 3.0
KINETIC_STEP = 0.12
VISCOSITY_REF = 0.25
VISCOSITY_POWER = 0.81
MACRO_STEP = 0.1
DIFFUSION = 1.6
HIGHEST = lax.Precision.HIGHEST


def coordinates(node_ids):
    along_x = node_ids // (NVY * NVZ)
    along_y = (node_ids // NVZ) % NVY
    along_z = node_ids % NVZ
    speed_x = -SPEED_LIMIT + (along_x.astype(jnp.float32) + 0.5) * (2.0 * SPEED_LIMIT / NVX)
    speed_y = -SPEED_LIMIT + (along_y.astype(jnp.float32) + 0.5) * (2.0 * SPEED_LIMIT / NVY)
    speed_z = -SPEED_LIMIT + (along_z.astype(jnp.float32) + 0.5) * (2.0 * SPEED_LIMIT / NVZ)
    return speed_x, speed_y, speed_z


def moment_rows(speed_x, speed_y, speed_z):
    weight = (2.0 * SPEED_LIMIT / NVX) * (2.0 * SPEED_LIMIT / NVY) * (2.0 * SPEED_LIMIT / NVZ) / (2.0 * math.pi) ** 1.5
    square = speed_x * speed_x + speed_y * speed_y + speed_z * speed_z
    unity = jnp.ones_like(speed_x)
    return weight * jnp.stack([unity, speed_x, speed_y, speed_z, square, speed_x * speed_x, speed_y * speed_y,
                               speed_x * speed_y, speed_x * speed_z, speed_y * speed_z,
                               speed_x * square, speed_y * square, speed_z * square])


def convert(moments):
    density = moments[0]
    vel_x = moments[1] / density
    vel_y = moments[2] / density
    vel_z = moments[3] / density
    twice_energy = moments[4]
    speed_sq = vel_x * vel_x + vel_y * vel_y + vel_z * vel_z
    temper = (twice_energy / density - speed_sq) / 3.0
    pressure = density * temper
    press_xx = moments[5]
    press_yy = moments[6]
    press_xy = moments[7]
    press_xz = moments[8]
    press_yz = moments[9]
    press_zz = twice_energy - press_xx - press_yy
    stress_xx = press_xx - density * vel_x * vel_x - pressure
    stress_yy = press_yy - density * vel_y * vel_y - pressure
    stress_xy = press_xy - density * vel_x * vel_y
    stress_xz = press_xz - density * vel_x * vel_z
    stress_yz = press_yz - density * vel_y * vel_z
    heat_x = 0.5 * (moments[10] - 2.0 * (vel_x * press_xx + vel_y * press_xy + vel_z * press_xz)
                    - vel_x * twice_energy + 2.0 * density * vel_x * speed_sq)
    heat_y = 0.5 * (moments[11] - 2.0 * (vel_x * press_xy + vel_y * press_yy + vel_z * press_yz)
                    - vel_y * twice_energy + 2.0 * density * vel_y * speed_sq)
    heat_z = 0.5 * (moments[12] - 2.0 * (vel_x * press_xz + vel_y * press_yz + vel_z * press_zz)
                    - vel_z * twice_energy + 2.0 * density * vel_z * speed_sq)
    return jnp.stack([density, moments[1], moments[2], moments[3], 0.5 * twice_energy,
                      stress_xx, stress_yy, stress_xy, stress_xz, stress_yz, heat_x, heat_y, heat_z])


def roll_z(values, offset):
    position = jnp.arange(values.shape[-1]) % NZ
    if offset == 1:
        return jnp.where(position == 0, jnp.roll(values, 1 - NZ, axis=-1), jnp.roll(values, 1, axis=-1))
    return jnp.where(position == NZ - 1, jnp.roll(values, NZ - 1, axis=-1), jnp.roll(values, -1, axis=-1))


def macro_step(state, extra):
    density = state[0]
    vel_x = state[1] / density
    vel_y = state[2] / density
    vel_z = state[3] / density
    energy = state[4]
    temper = (2.0 / 3.0) * (energy / density - 0.5 * (vel_x * vel_x + vel_y * vel_y + vel_z * vel_z))
    pressure = density * temper
    stress_xx, stress_yy, stress_xy, stress_xz, stress_yz = extra[0], extra[1], extra[2], extra[3], extra[4]
    stress_zz = -stress_xx - stress_yy
    enthalpy = energy + pressure
    flux_x = jnp.stack([state[1], state[1] * vel_x + pressure + stress_xx, state[2] * vel_x + stress_xy,
                        state[3] * vel_x + stress_xz,
                        enthalpy * vel_x + stress_xx * vel_x + stress_xy * vel_y + stress_xz * vel_z + extra[5]])
    flux_y = jnp.stack([state[2], state[1] * vel_y + stress_xy, state[2] * vel_y + pressure + stress_yy,
                        state[3] * vel_y + stress_yz,
                        enthalpy * vel_y + stress_xy * vel_x + stress_yy * vel_y + stress_yz * vel_z + extra[6]])
    flux_z = jnp.stack([state[3], state[1] * vel_z + stress_xz, state[2] * vel_z + stress_yz,
                        state[3] * vel_z + pressure + stress_zz,
                        enthalpy * vel_z + stress_xz * vel_x + stress_yz * vel_y + stress_zz * vel_z + extra[7]])
    div_x = 0.5 * (flux_x[:, 2:] - flux_x[:, :-2])
    div_y = 0.5 * (jnp.roll(flux_y, -NZ, axis=-1) - jnp.roll(flux_y, NZ, axis=-1))[:, 1:-1]
    div_z = 0.5 * (roll_z(flux_z, -1) - roll_z(flux_z, 1))[:, 1:-1]
    center = state[:, 1:-1]
    beside = (jnp.roll(state, -NZ, axis=-1) + jnp.roll(state, NZ, axis=-1) + roll_z(state, -1) + roll_z(state, 1))[:, 1:-1]
    spread = state[:, 2:] + state[:, :-2] + beside - 6.0 * center
    return center - MACRO_STEP * (div_x + div_y + div_z) + DIFFUSION * MACRO_STEP * spread


def equilibrium(speeds, macro, heat):
    density = macro[0]
    vel_x = macro[1] / density
    vel_y = macro[2] / density
    vel_z = macro[3] / density
    temper = (2.0 / 3.0) * (macro[4] / density - 0.5 * (vel_x * vel_x + vel_y * vel_y + vel_z * vel_z))
    rel_x = speeds[0][:, None, None] - vel_x[None]
    rel_y = speeds[1][:, None, None] - vel_y[None]
    rel_z = speeds[2][:, None, None] - vel_z[None]
    rel_sq = rel_x * rel_x + rel_y * rel_y + rel_z * rel_z
    along = rel_x * heat[0][None] + rel_y * heat[1][None] + rel_z * heat[2][None]
    shakhov = 1.0 + (1.0 - PRANDTL) * along * (rel_sq / temper - 5.0) / (5.0 * density * temper * temper)
    return density * temper ** -1.5 * jnp.exp(-rel_sq / (2.0 * temper)) * shakhov


def relax_rate(macro):
    density = macro[0]
    vel_x = macro[1] / density
    vel_y = macro[2] / density
    vel_z = macro[3] / density
    temper = (2.0 / 3.0) * (macro[4] / density - 0.5 * (vel_x * vel_x + vel_y * vel_y + vel_z * vel_z))
    return KINETIC_STEP * density * temper ** (1.0 - VISCOSITY_POWER) / VISCOSITY_REF


def warming(center, minus_one, minus_two, plus_one, plus_two, courant):
    ahead = jnp.maximum(courant, 0.0)
    behind = jnp.maximum(-courant, 0.0)
    return (ahead * 0.5 * (3.0 * center - 4.0 * minus_one + minus_two)
            - ahead * ahead * 0.5 * (center - 2.0 * minus_one + minus_two)
            + behind * 0.5 * (3.0 * center - 4.0 * plus_one + plus_two)
            - behind * behind * 0.5 * (center - 2.0 * plus_one + plus_two))


def kinetic(padded, speeds, feq, rate, inflow_dist, inflow_mask):
    center = padded[:, 2:-2]
    adv_x = warming(center, padded[:, 1:-3], padded[:, :-4], padded[:, 3:-1], padded[:, 4:],
                    KINETIC_STEP * speeds[0][:, None, None])
    adv_y = warming(center, jnp.roll(center, NZ, axis=-1), jnp.roll(center, 2 * NZ, axis=-1),
                    jnp.roll(center, -NZ, axis=-1), jnp.roll(center, -2 * NZ, axis=-1),
                    KINETIC_STEP * speeds[1][:, None, None])
    back_one = roll_z(center, 1)
    front_one = roll_z(center, -1)
    adv_z = warming(center, back_one, roll_z(back_one, 1), front_one, roll_z(front_one, -1),
                    KINETIC_STEP * speeds[2][:, None, None])
    updated = center - (adv_x + adv_y + adv_z) + rate[None] * (feq - center)
    return jnp.where(inflow_mask[None] == 1, inflow_dist[:, None, None], updated)


def inflow_values(speeds, inflow_scalars, inflow_drift):
    rel_x = speeds[0] - inflow_drift[0]
    rel_y = speeds[1] - inflow_drift[1]
    rel_z = speeds[2] - inflow_drift[2]
    rel_sq = rel_x * rel_x + rel_y * rel_y + rel_z * rel_z
    return inflow_scalars[0] * inflow_scalars[1] ** -1.5 * jnp.exp(-rel_sq / (2.0 * inflow_scalars[1]))


def macro_solve(fields):
    extra = jnp.pad(fields[5:], ((0, 0), (1, 1), (0, 0)), mode="edge")
    state = fields[:5]
    for substep in range(MSTEPS):
        state = macro_step(jnp.pad(state, ((0, 0), (1, 1), (0, 0)), mode="edge"), extra)
    return state


def reference(distribution, block_map, inflow_mask, owner_map, inflow_scalars, inflow_drift):
    width = NY * NZ
    node_ids = (block_map[:, None] * VB + jnp.arange(VB, dtype=jnp.int32)[None, :]).reshape(-1).astype(jnp.int32)
    speeds = coordinates(node_ids)
    rows = moment_rows(*speeds)
    inflow_dist = inflow_values(speeds, inflow_scalars, inflow_drift)
    current = distribution
    macro = None
    for iteration in range(ITERS):
        moments = jnp.dot(rows, current.reshape(V, NXC * width), precision=HIGHEST).reshape(13, NXC, width)
        fields = convert(moments)
        macro = macro_solve(fields)
        heat = fields[10:13]
        rate = relax_rate(macro)

        def advance(group, macro=macro, heat=heat, rate=rate):
            group_dist, group_x, group_y, group_z, group_inflow = group
            lower = jnp.broadcast_to(group_inflow[:, None, None], (VB, 2, width))
            upper = jnp.repeat(group_dist[:, -1:], 2, axis=1)
            padded = jnp.concatenate([lower, group_dist, upper], axis=1)
            group_speeds = (group_x, group_y, group_z)
            feq = equilibrium(group_speeds, macro, heat)
            return kinetic(padded, group_speeds, feq, rate, group_inflow, inflow_mask)

        current = lax.map(advance, (current.reshape(NB, VB, NXC, width), speeds[0].reshape(NB, VB),
                                    speeds[1].reshape(NB, VB), speeds[2].reshape(NB, VB),
                                    inflow_dist.reshape(NB, VB))).reshape(V, NXC, width)
    blocks = macro.reshape(5, N_SPACE, N_VEL, OB)
    ordered = jnp.take(blocks, owner_map, axis=2).reshape(5, NXC * width)
    return current, ordered
```

```python
import functools
import math

import jax
import jax.numpy as jnp
from jax import lax
from jax.experimental import pallas as pl
from jax.experimental.pallas import tpu as pltpu
from jax.sharding import PartitionSpec as P

NVX = 32
NVY = 32
NVZ = 16
VB = 128
NZ = 16
MSTEPS = 4

SPEED_LIMIT = 3.5
KINETIC_STEP = 0.12
VISCOSITY_REF = 0.25
VISCOSITY_POWER = 0.81
MACRO_STEP = 0.1
DIFFUSION = 1.6

DX = 2.0 * SPEED_LIMIT / NVX
DY = 2.0 * SPEED_LIMIT / NVY
DZ = 2.0 * SPEED_LIMIT / NVZ
WEIGHT = DX * DY * DZ / (2.0 * math.pi) ** 1.5
ROWS = VB // NVZ
PARTS = NVY // ROWS
SUB = 8
LANES = 128
VMEM_LIMIT = 60 << 20
AHEAD = 4


def speed(index, spacing):
    return -SPEED_LIMIT + (index + 0.5) * spacing


def upwind(courant):
    return 1.5 * courant - 0.5 * courant * courant, courant * courant - 2.0 * courant, 0.5 * courant - 0.5 * courant * courant


def slot_sizes(blocks):
    first = max(1, blocks // 2)
    second = min(blocks // 4, blocks - first)
    return first, second, blocks - first - second


def block_speeds(block):
    along_x = (block // PARTS).astype(jnp.float32)
    base_y = ((block % PARTS) * ROWS).astype(jnp.float32)
    return speed(along_x, DX), speed(base_y, DY)


def sublane(shift):
    return lambda x: pltpu.roll(x, shift % SUB, 0)


def lane(shift):
    return lambda x: pltpu.roll(x, shift % LANES, 1)


def places():
    plane = lax.broadcasted_iota(jnp.int32, (SUB, LANES), 0) % 4
    spot = lax.broadcasted_iota(jnp.int32, (SUB, LANES), 1)
    return plane, spot, spot % NZ


def gather_kernel(sizes, bm_ref, f_hbm, mom_ref, *refs):
    kinds = sum(1 for s in sizes if s)
    up = refs[:kinds]
    down = refs[kinds:2 * kinds]
    fbuf, pack, acc, in_sem, out_sem = refs[2 * kinds:]
    blocks = bm_ref.shape[0]
    plane, _, _ = places()
    high = plane >= 2
    half = PARTS * NVX // 2
    offsets = [0]
    for s in sizes[:kinds]:
        offsets.append(offsets[-1] + s)

    def fetch(i):
        return pltpu.make_async_copy(f_hbm.at[pl.ds(i * VB, VB)], fbuf.at[pl.ds(i * VB, VB)], in_sem.at[i])

    for i in range(min(AHEAD, blocks)):
        fetch(i).start()
    for r in range(13):
        acc[r] = jnp.zeros((SUB, LANES), jnp.float32)

    def step(i, positives):
        @pl.when(i + AHEAD < blocks)
        def _():
            fetch(i + AHEAD).start()
        fetch(i).wait()
        block = bm_ref[i]
        positive = block >= half
        cx, cy0 = block_speeds(block)

        def row(upward):
            def body(y, carry):
                cy = cy0 + y.astype(jnp.float32) * DY
                s0 = s1 = s2 = s3 = None
                for e in range(NVZ // 2):
                    a = fbuf[i * VB + y * NVZ + e]
                    b = fbuf[i * VB + y * NVZ + e + NVZ // 2]
                    if upward:
                        pack[i * (VB // 2) + y * (NVZ // 2) + e] = jnp.where(high, sublane(4)(a), sublane(2)(b))
                    else:
                        pack[i * (VB // 2) + y * (NVZ // 2) + e] = jnp.where(high, sublane(6)(b), sublane(4)(a))
                for e in range(NVZ // 2, NVZ):
                    z = speed(e, DZ)
                    a = fbuf[i * VB + y * NVZ + e]
                    b = fbuf[i * VB + y * NVZ + NVZ - 1 - e]
                    p = a + b
                    m = (a - b) * z
                    if s0 is None:
                        s0, s1, s2, s3 = p, m, p * (z * z), m * (z * z)
                    else:
                        s0, s1, s2, s3 = s0 + p, s1 + m, s2 + p * (z * z), s3 + m * (z * z)
                a0, a1, a2, a3, b0, b1, b2, c0, c1, d0 = carry
                t1 = s0 * cy
                t2 = t1 * cy
                u1 = s1 * cy
                return (a0 + s0, a1 + t1, a2 + t2, a3 + t2 * cy, b0 + s1, b1 + u1, b2 + u1 * cy, c0 + s2, c1 + s2 * cy, d0 + s3)

            zero = jnp.zeros((SUB, LANES), jnp.float32)
            a0, a1, a2, a3, b0, b1, b2, c0, c1, d0 = lax.fori_loop(0, ROWS, body, (zero,) * 10)
            x0 = a0 * cx
            xx = x0 * cx
            square = xx + a2 + c0
            terms = (a0, x0, a1, b0, square, xx, a2, a1 * cx, b0 * cx, b1, square * cx,
                     a1 * (cx * cx) + a3 + c1, b0 * (cx * cx) + b2 + d0)
            for r, term in enumerate(terms):
                acc[r] = acc[r] + term

        rank = jnp.where(positive, positives, i - positives)
        for upward in (True, False):
            @pl.when(positive if upward else jnp.logical_not(positive))
            def _(upward=upward):
                row(upward)
                for kind in range(kinds):
                    @pl.when(jnp.logical_and(rank >= offsets[kind], rank < offsets[kind + 1]))
                    def _(kind=kind):
                        target = (up if upward else down)[kind]
                        pltpu.make_async_copy(pack.at[pl.ds(i * (VB // 2), VB // 2)],
                                              target.at[pl.ds((rank - offsets[kind]) * (VB // 2), VB // 2)],
                                              out_sem.at[i]).start()
        return positives + jnp.where(positive, 1, 0)

    positives = lax.fori_loop(0, blocks, step, jnp.int32(0))
    for r in range(13):
        mom_ref[r] = acc[r] * WEIGHT
    limit = sizes[0] + sizes[1]
    excess = jnp.where(jnp.maximum(positives, blocks - positives) > limit, 1.0, 0.0)
    mom_ref[13] = jnp.full((SUB, LANES), excess, jnp.float32)

    def drain(i, carry):
        pltpu.make_async_copy(pack.at[pl.ds(i * (VB // 2), VB // 2)], up[0].at[pl.ds(0, VB // 2)], out_sem.at[i]).wait()
        return carry

    lax.fori_loop(0, blocks, drain, 0)


def gather(f, block_map, sizes):
    blocks = block_map.shape[0]
    half = VB // 2
    bufs = [jax.ShapeDtypeStruct((s * half, SUB, LANES), jnp.float32) for s in sizes if s]
    outs = pl.pallas_call(
        functools.partial(gather_kernel, sizes),
        in_specs=[pl.BlockSpec(memory_space=pltpu.SMEM), pl.BlockSpec(memory_space=pl.ANY)],
        out_specs=[pl.BlockSpec(memory_space=pltpu.VMEM)] + [pl.BlockSpec(memory_space=pl.ANY)] * (2 * len(bufs)),
        out_shape=[jax.ShapeDtypeStruct((14, SUB, LANES), jnp.float32)] + bufs + bufs,
        scratch_shapes=[pltpu.VMEM((blocks * VB, SUB, LANES), jnp.float32),
                        pltpu.VMEM((blocks * half, SUB, LANES), jnp.float32),
                        pltpu.VMEM((13, SUB, LANES), jnp.float32),
                        pltpu.SemaphoreType.DMA((blocks,)), pltpu.SemaphoreType.DMA((blocks,))],
        compiler_params=pltpu.CompilerParams(vmem_limit_bytes=VMEM_LIMIT),
        name="gather",
    )(block_map, f)
    n = len(bufs)
    return outs[0], outs[1:1 + n], outs[1 + n:]


def convert(m):
    inv = 1.0 / m[0]
    ux, uy, uz = m[1] * inv, m[2] * inv, m[3] * inv
    sq = ux * ux + uy * uy + uz * uz
    density = m[0]
    pressure = density * ((m[4] * inv - sq) / 3.0)
    xx, yy, xy, xz, yz = m[5:10]
    zz = m[4] - xx - yy
    sxx = xx - density * ux * ux - pressure
    syy = yy - density * uy * uy - pressure
    sxy = xy - density * ux * uy
    sxz = xz - density * ux * uz
    syz = yz - density * uy * uz
    hx = 0.5 * (m[10] - 2.0 * (ux * xx + uy * xy + uz * xz) - ux * m[4] + 2.0 * density * ux * sq)
    hy = 0.5 * (m[11] - 2.0 * (ux * xy + uy * yy + uz * yz) - uy * m[4] + 2.0 * density * uy * sq)
    hz = 0.5 * (m[12] - 2.0 * (ux * xz + uy * yz + uz * zz) - uz * m[4] + 2.0 * density * uz * sq)
    return [density, m[1], m[2], m[3], 0.5 * m[4]], [sxx, syy, sxy, sxz, syz, hx, hy, hz]


def primitive(state):
    density = state[0]
    inv = 1.0 / density
    ux, uy, uz = state[1] * inv, state[2] * inv, state[3] * inv
    temper = (2.0 / 3.0) * (state[4] * inv - 0.5 * (ux * ux + uy * uy + uz * uz))
    return density, ux, uy, uz, temper


def fluxes(state, extra):
    density, ux, uy, uz, temper = primitive(state)
    pressure = density * temper
    sxx, syy, sxy, sxz, syz, hx, hy, hz = extra
    szz = -sxx - syy
    enthalpy = state[4] + pressure
    fx = [state[1], state[1] * ux + pressure + sxx, state[2] * ux + sxy, state[3] * ux + sxz,
          enthalpy * ux + sxx * ux + sxy * uy + sxz * uz + hx]
    fy = [state[2], state[1] * uy + sxy, state[2] * uy + pressure + syy, state[3] * uy + syz,
          enthalpy * uy + sxy * ux + syy * uy + syz * uz + hy]
    fz = [state[3], state[1] * uz + sxz, state[2] * uz + syz, state[3] * uz + pressure + szz,
          enthalpy * uz + sxz * ux + syz * uy + szz * uz + hz]
    return fx, fy, fz


def macro_kernel(low_ref, own_ref, high_ref, macro_ref, cell_ref):
    plane, spot, along_z = places()
    index = lax.axis_index("space")
    count = lax.axis_size("space")
    first = (plane + index) == 0
    last = (plane + (count - 1 - index)) == 3
    last = jnp.logical_and(last, plane == 3)
    states, extras = [], []
    for ref in (low_ref, own_ref, high_ref):
        state, extra = convert([ref[r] for r in range(13)])
        states.append(state)
        extras.append(extra)

    def from_below(slabs):
        low, own, high = slabs
        a = sublane(1)(low)
        b = sublane(1)(jnp.where(plane == 3, sublane(4)(low), own))
        c = sublane(1)(jnp.where(plane == 3, sublane(4)(own), high))
        return [a, jnp.where(first, own, b), c]

    def from_above(slabs):
        low, own, high = slabs
        a = sublane(-1)(jnp.where(plane == 0, sublane(4)(own), low))
        b = sublane(-1)(jnp.where(plane == 0, sublane(4)(high), own))
        c = sublane(-1)(high)
        return [a, jnp.where(last, own, b), c]

    def y_minus(x):
        return lane(NZ)(jnp.where(spot >= LANES - NZ, sublane(4)(x), x))

    def y_plus(x):
        return lane(-NZ)(jnp.where(spot < NZ, sublane(4)(x), x))

    def z_minus(x):
        return lane(1)(jnp.where(along_z == NZ - 1, lane(-NZ)(x), x))

    def z_plus(x):
        return lane(-1)(jnp.where(along_z == 0, lane(NZ)(x), x))

    mix = DIFFUSION * MACRO_STEP
    push = 0.5 * MACRO_STEP
    for _ in range(MSTEPS):
        flux = [fluxes(s, e) for s, e in zip(states, extras)]
        fresh = [[], [], []]
        for r in range(5):
            scaled = [mix * states[k][r] for k in range(3)]
            xp = from_above([scaled[k] - push * flux[k][0][r] for k in range(3)])
            xm = from_below([scaled[k] + push * flux[k][0][r] for k in range(3)])
            for k in range(3):
                gy = push * flux[k][1][r]
                gz = push * flux[k][2][r]
                total = (1.0 - 6.0 * mix) * states[k][r] + xp[k] + xm[k]
                total = total + (y_plus(scaled[k] - gy) + y_minus(scaled[k] + gy))
                total = total + (z_plus(scaled[k] - gz) + z_minus(scaled[k] + gz))
                fresh[k].append(total)
        states = fresh
    state = states[1]
    for r in range(5):
        macro_ref[r] = state[r]
    density, ux, uy, uz, temper = primitive(state)
    logt = jnp.log(temper)
    rate = (KINETIC_STEP / VISCOSITY_REF) * density * jnp.exp((1.0 - VISCOSITY_POWER) * logt)
    skew = 1.0 / (15.0 * density * temper * temper)
    cell_ref[0] = ux
    cell_ref[1] = uy
    cell_ref[2] = uz
    cell_ref[3] = 0.5 / temper
    cell_ref[4] = rate * density * jnp.exp(-1.5 * logt)
    cell_ref[5] = extras[1][5] * skew
    cell_ref[6] = extras[1][6] * skew
    cell_ref[7] = extras[1][7] * skew
    cell_ref[8] = 1.0 - rate


def macro_solve(low, own, high):
    return pl.pallas_call(
        macro_kernel,
        out_shape=[jax.ShapeDtypeStruct((5, SUB, LANES), jnp.float32), jax.ShapeDtypeStruct((9, SUB, LANES), jnp.float32)],
        compiler_params=pltpu.CompilerParams(vmem_limit_bytes=VMEM_LIMIT),
        name="macro",
    )(low, own, high)


def kinetic_kernel(spans, aliased, bm_ref, scal_ref, drift_ref, mask_ref, cell_ref, f_hbm, *refs):
    kinds = len(spans)
    up = refs[:kinds]
    down = refs[kinds:2 * kinds]
    refs = refs[2 * kinds + (1 if aliased else 0):]
    out_hbm, fbuf, hbuf, gz_ref, az_ref, sz_ref, iz_ref, pick, in_sem, halo_sem, out_sem = refs
    blocks = bm_ref.shape[0]
    low_slot = spans[0][0]
    high_slot = spans[-1][1]
    half_id = PARTS * NVX // 2
    half = VB // 2
    index = lax.axis_index("space")
    count = lax.axis_size("space")

    def choose(i, carry):
        chosen, positives = carry
        positive = bm_ref[i] >= half_id
        rank = jnp.where(positive, positives, i - positives)
        take = jnp.logical_and(rank >= low_slot, rank < high_slot)

        @pl.when(take)
        def _():
            pick[0, chosen] = i
            pick[1, chosen] = rank
        return chosen + jnp.where(take, 1, 0), positives + jnp.where(positive, 1, 0)

    chosen, _ = lax.fori_loop(0, blocks, choose, (jnp.int32(0), jnp.int32(0)))

    def fetch(n):
        i = pick[0, n]
        return pltpu.make_async_copy(f_hbm.at[pl.ds(i * VB, VB)], fbuf.at[pl.ds(i * VB, VB)], in_sem.at[i])

    def begin(n):
        fetch(n).start()
        i = pick[0, n]
        rank = pick[1, n]
        positive = bm_ref[i] >= half_id
        for upward in (True, False):
            for kind, (lo, hi) in enumerate(spans):
                here = jnp.logical_and(rank >= lo, rank < hi)

                @pl.when(jnp.logical_and(here, positive if upward else jnp.logical_not(positive)))
                def _(upward=upward, kind=kind, lo=lo):
                    source = (up if upward else down)[kind]
                    pltpu.make_async_copy(source.at[pl.ds((rank - lo) * half, half)], hbuf.at[pl.ds(i * half, half)],
                                          halo_sem.at[i]).start()

    for n in range(min(AHEAD, blocks)):
        @pl.when(n < chosen)
        def _(n=n):
            begin(n)

    plane, spot, along_z = places()
    fixed = mask_ref[...] == 1
    ux, uy, uz, inv2t = cell_ref[0], cell_ref[1], cell_ref[2], cell_ref[3]
    hot = jnp.full((SUB, LANES), scal_ref[1], jnp.float32)
    hot_inv = 0.5 / hot
    hot_scale = scal_ref[0] * jnp.exp(-1.5 * jnp.log(hot))
    for e in range(NVZ):
        cz = speed(e, DZ)
        rel = cz - uz
        t = rel * rel * inv2t
        gz_ref[e] = jnp.exp(-t)
        sz_ref[e] = 2.0 * t
        az_ref[e] = rel * cell_ref[7]
        off = cz - drift_ref[2]
        iz_ref[e] = jnp.exp(-(off * off) * hot_inv)

    def run(n, carry):
        @pl.when(n + AHEAD < chosen)
        def _():
            begin(n + AHEAD)
        i = pick[0, n]
        block = bm_ref[i]
        positive = block >= half_id
        y_positive = (block % PARTS) >= PARTS // 2
        cx, cy0 = block_speeds(block)
        fetch(n).wait()
        pltpu.make_async_copy(up[0].at[pl.ds(0, half)], hbuf.at[pl.ds(i * half, half)], halo_sem.at[i]).wait()
        k0x, k1x, k2x = upwind(KINETIC_STEP * jnp.abs(cx))
        relx = cx - ux
        tx = relx * relx * inv2t
        ax = relx * cell_ref[5]
        offx = cx - drift_ref[0]

        def rows(x_up, edge, y_up):
            def body(y, carry):
                cy = cy0 + y.astype(jnp.float32) * DY
                k0y, k1y, k2y = upwind(KINETIC_STEP * jnp.abs(cy))
                rely = cy - uy
                txy = tx + rely * rely * inv2t
                axy = ax + rely * cell_ref[6]
                gxy = cell_ref[4] * jnp.exp(-txy)
                sxy = 2.0 * txy - 5.0
                keep = cell_ref[8] - (k0x + k0y)
                offy = cy - drift_ref[1]
                ixy = hot_scale * jnp.exp(-(offx * offx + offy * offy) * hot_inv)
                for e in range(NVZ):
                    k0z, k1z, k2z = upwind(KINETIC_STEP * abs(speed(e, DZ)))
                    spot_v = i * VB + y * NVZ + e
                    f = fbuf[spot_v]
                    inflow = ixy * iz_ref[e]
                    total = f * (keep - k0z)
                    if edge and x_up:
                        halo = inflow
                    elif not edge:
                        halo = hbuf[i * half + y * (NVZ // 2) + e % (NVZ // 2)]
                        if e >= NVZ // 2:
                            halo = sublane(2 if x_up else -2)(halo)
                    else:
                        halo = jnp.where(plane == 0, sublane(1)(f), sublane(2)(f))
                    if x_up:
                        x1 = sublane(1)(jnp.where(plane == 3, halo, f))
                        x2 = sublane(2)(jnp.where(plane >= 2, halo, f))
                    else:
                        x1 = sublane(-1)(jnp.where(plane == 0, halo, f))
                        x2 = sublane(-2)(jnp.where(plane < 2, halo, f))
                    total = total - k1x * x1 - k2x * x2
                    across = sublane(4)(f)
                    if y_up:
                        y1 = lane(NZ)(jnp.where(spot >= LANES - NZ, across, f))
                        y2 = lane(2 * NZ)(jnp.where(spot >= LANES - 2 * NZ, across, f))
                    else:
                        y1 = lane(-NZ)(jnp.where(spot < NZ, across, f))
                        y2 = lane(-2 * NZ)(jnp.where(spot < 2 * NZ, across, f))
                    total = total - k1y * y1 - k2y * y2
                    if e >= NVZ // 2:
                        wrap = lane(-NZ)(f)
                        z1 = lane(1)(jnp.where(along_z == NZ - 1, wrap, f))
                        z2 = lane(2)(jnp.where(along_z >= NZ - 2, wrap, f))
                    else:
                        wrap = lane(NZ)(f)
                        z1 = lane(-1)(jnp.where(along_z == 0, wrap, f))
                        z2 = lane(-2)(jnp.where(along_z < 2, wrap, f))
                    total = total - k1z * z1 - k2z * z2
                    shape = 1.0 + (axy + az_ref[e]) * (sxy + sz_ref[e])
                    total = total + (gxy * gz_ref[e]) * shape
                    fbuf[spot_v] = jnp.where(fixed, inflow, total)
                return carry

            lax.fori_loop(0, ROWS, body, 0)

        for x_up in (True, False):
            outer = (index == 0) if x_up else (index == count - 1)
            for edge in (True, False):
                for y_up in (True, False):
                    flag = jnp.logical_and(positive if x_up else jnp.logical_not(positive),
                                           outer if edge else jnp.logical_not(outer))
                    flag = jnp.logical_and(flag, y_positive if y_up else jnp.logical_not(y_positive))

                    @pl.when(flag)
                    def _(x_up=x_up, edge=edge, y_up=y_up):
                        rows(x_up, edge, y_up)
        pltpu.make_async_copy(fbuf.at[pl.ds(i * VB, VB)], out_hbm.at[pl.ds(i * VB, VB)], out_sem.at[i]).start()
        return carry

    lax.fori_loop(0, chosen, run, 0)

    def drain(n, carry):
        i = pick[0, n]
        pltpu.make_async_copy(fbuf.at[pl.ds(i * VB, VB)], out_hbm.at[pl.ds(i * VB, VB)], out_sem.at[i]).wait()
        return carry

    lax.fori_loop(0, chosen, drain, 0)


def kinetic(f, block_map, scalars, drift, mask, cells, spans, up, down, into=None):
    blocks = block_map.shape[0]
    half = VB // 2
    smem = pl.BlockSpec(memory_space=pltpu.SMEM)
    vmem = pl.BlockSpec(memory_space=pltpu.VMEM)
    hbm = pl.BlockSpec(memory_space=pl.ANY)
    operands = [block_map, scalars, drift, mask, cells, f, *up, *down]
    specs = [smem, smem, smem, vmem, vmem, hbm] + [hbm] * (len(up) + len(down))
    aliases = {}
    if into is not None:
        aliases = {len(operands): 0}
        operands.append(into)
        specs.append(hbm)
    table = pltpu.VMEM((NVZ, SUB, LANES), jnp.float32)
    return pl.pallas_call(
        functools.partial(kinetic_kernel, spans, into is not None),
        in_specs=specs,
        out_specs=hbm,
        out_shape=jax.ShapeDtypeStruct(f.shape, jnp.float32),
        scratch_shapes=[pltpu.VMEM((blocks * VB, SUB, LANES), jnp.float32), pltpu.VMEM((blocks * half, SUB, LANES), jnp.float32),
                        table, table, table, table, pltpu.SMEM((2, blocks), jnp.int32),
                        pltpu.SemaphoreType.DMA((blocks,)), pltpu.SemaphoreType.DMA((blocks,)), pltpu.SemaphoreType.DMA((blocks,))],
        input_output_aliases=aliases,
        compiler_params=pltpu.CompilerParams(vmem_limit_bytes=VMEM_LIMIT),
        name="kinetic",
    )(*operands)


def over_vel(values):
    count = lax.axis_size("vel")
    if count & (count - 1):
        return lax.psum(values, "vel")
    reach = 1
    while reach < count:
        values = values + lax.ppermute(values, "vel", [(i, i ^ reach) for i in range(count)])
        reach *= 2
    return values


def tiles(array):
    lead, planes, width = array.shape
    return array.reshape(lead, planes, width // LANES, LANES).transpose(0, 2, 1, 3).reshape(lead, planes * width // LANES, LANES)


def per_device(distribution, block_map, inflow_mask, owner_map, inflow_scalars, inflow_drift):
    vel_count = lax.axis_size("vel")
    vel_index = lax.axis_index("vel")
    space_count = lax.axis_size("space")
    local_vel, planes, width = distribution.shape
    assert planes == MSTEPS and planes * width == SUB * LANES
    block_len = planes * width // vel_count
    blocks = block_map.shape[0]
    sizes = slot_sizes(blocks)
    f = tiles(distribution)
    mask = tiles(inflow_mask[None])[0]
    rise = [(i, i + 1) for i in range(space_count - 1)]
    fall = [(i + 1, i) for i in range(space_count - 1)]

    partial, ups, downs = gather(f, block_map, sizes)
    got_up = [lax.ppermute(ups[0], "space", rise)]
    got_down = [lax.ppermute(downs[0], "space", fall)]
    if sizes[1]:
        got_up.append(lax.ppermute(ups[1], "space", rise))
        got_down.append(lax.ppermute(downs[1], "space", fall))
    total = over_vel(partial)
    low = lax.ppermute(total[:13], "space", rise)
    high = lax.ppermute(total[:13], "space", fall)
    macro, cells = macro_solve(low, total, high)
    common = (f, block_map, inflow_scalars, inflow_drift, mask, cells)
    updated = kinetic(*common, ((0, sizes[0]),), got_up[:1], got_down[:1])
    if sizes[1]:
        edge = sizes[0] + sizes[1]
        spans = ((sizes[0], edge),)
        if sizes[2]:
            spans = spans + ((edge, blocks),)
            extra = lax.cond(total[13, 0, 0] > 0.5,
                             lambda a, b: (lax.ppermute(a, "space", rise), lax.ppermute(b, "space", fall)),
                             lambda a, b: (a, b), ups[2], downs[2])
            got_up.append(extra[0])
            got_down.append(extra[1])
        updated = kinetic(*common, spans, got_up[1:], got_down[1:], into=updated)
    current = updated.reshape(local_vel, width // LANES, planes, LANES).transpose(0, 2, 1, 3).reshape(local_vel, planes, width)
    flat = macro.reshape(5, width // LANES, planes, LANES).transpose(0, 2, 1, 3).reshape(5, vel_count, block_len)
    mine = lax.dynamic_slice_in_dim(flat, owner_map[vel_index], 1, axis=1).reshape(5, block_len)
    return (current, mine)


def solution(mesh):
    return jax.shard_map(
        per_device,
        mesh=mesh,
        in_specs=(P("vel", "space", None), P("vel"), P("space", None), P(), P(), P()),
        out_specs=(P("vel", "space", None), P(None, ("space", "vel"))),
        check_vma=False,
    )
```

```python
import functools
import math

import jax
import jax.numpy as jnp
from jax import lax
from jax.experimental import pallas as pl
from jax.experimental.pallas import tpu as pltpu
from jax.sharding import PartitionSpec as P

NVX = 32
NVY = 32
NVZ = 16
VB = 128
NZ = 16
MSTEPS = 4

SPEED_LIMIT = 3.5
KINETIC_STEP = 0.12
VISCOSITY_REF = 0.25
VISCOSITY_POWER = 0.81
MACRO_STEP = 0.1
DIFFUSION = 1.6

DX = 2.0 * SPEED_LIMIT / NVX
DY = 2.0 * SPEED_LIMIT / NVY
DZ = 2.0 * SPEED_LIMIT / NVZ
WEIGHT = DX * DY * DZ / (2.0 * math.pi) ** 1.5
ROWS = VB // NVZ
PARTS = NVY // ROWS
SUB = 8
LANES = 128
VMEM_LIMIT = 67_000_000
SMALL_LIMIT = 16 << 20
AHEAD = 16


def speed(index, spacing):
    return -SPEED_LIMIT + (index + 0.5) * spacing


def upwind(courant):
    return 1.5 * courant - 0.5 * courant * courant, courant * courant - 2.0 * courant, 0.5 * courant - 0.5 * courant * courant


def slot_sizes(blocks):
    first = max(1, blocks // 2)
    second = min(blocks // 4, blocks - first)
    return first, second, blocks - first - second


def block_speeds(block):
    along_x = (block // PARTS).astype(jnp.float32)
    base_y = ((block % PARTS) * ROWS).astype(jnp.float32)
    return speed(along_x, DX), speed(base_y, DY)


def sublane(shift):
    return lambda x: pltpu.roll(x, shift % SUB, 0)


def lane(shift):
    return lambda x: pltpu.roll(x, shift % LANES, 1)


def places():
    plane = lax.broadcasted_iota(jnp.int32, (SUB, LANES), 0) % 4
    spot = lax.broadcasted_iota(jnp.int32, (SUB, LANES), 1)
    return plane, spot, spot % NZ


def gather_kernel(sizes, bm_ref, f_hbm, mom_ref, *refs):
    kinds = sum(1 for s in sizes if s)
    up = refs[:kinds]
    down = refs[kinds:2 * kinds]
    fbuf, pack, acc, in_sem, out_sem = refs[2 * kinds:]
    blocks = bm_ref.shape[0]
    plane, _, _ = places()
    high = plane >= 2
    half = PARTS * NVX // 2
    offsets = [0]
    for s in sizes[:kinds]:
        offsets.append(offsets[-1] + s)

    def fetch(i):
        return pltpu.make_async_copy(f_hbm.at[pl.ds(i * VB, VB)], fbuf.at[pl.ds(i * VB, VB)], in_sem.at[i])

    for i in range(min(AHEAD, blocks)):
        fetch(i).start()
    for r in range(13):
        acc[r] = jnp.zeros((SUB, LANES), jnp.float32)

    def step(i, positives):
        @pl.when(i + AHEAD < blocks)
        def _():
            fetch(i + AHEAD).start()
        fetch(i).wait()
        block = bm_ref[i]
        positive = block >= half
        cx, cy0 = block_speeds(block)

        def row(upward):
            def body(y, carry):
                cy = cy0 + y.astype(jnp.float32) * DY
                s0 = s1 = s2 = s3 = None
                for e in range(NVZ // 2):
                    a = fbuf[i * VB + y * NVZ + e]
                    b = fbuf[i * VB + y * NVZ + e + NVZ // 2]
                    if upward:
                        pack[i * (VB // 2) + y * (NVZ // 2) + e] = jnp.where(high, sublane(4)(a), sublane(2)(b))
                    else:
                        pack[i * (VB // 2) + y * (NVZ // 2) + e] = jnp.where(high, sublane(6)(b), sublane(4)(a))
                for e in range(NVZ // 2, NVZ):
                    z = speed(e, DZ)
                    a = fbuf[i * VB + y * NVZ + e]
                    b = fbuf[i * VB + y * NVZ + NVZ - 1 - e]
                    p = a + b
                    m = (a - b) * z
                    if s0 is None:
                        s0, s1, s2, s3 = p, m, p * (z * z), m * (z * z)
                    else:
                        s0, s1, s2, s3 = s0 + p, s1 + m, s2 + p * (z * z), s3 + m * (z * z)
                a0, a1, a2, a3, b0, b1, b2, c0, c1, d0 = carry
                t1 = s0 * cy
                t2 = t1 * cy
                u1 = s1 * cy
                return (a0 + s0, a1 + t1, a2 + t2, a3 + t2 * cy, b0 + s1, b1 + u1, b2 + u1 * cy, c0 + s2, c1 + s2 * cy, d0 + s3)

            zero = jnp.zeros((SUB, LANES), jnp.float32)
            a0, a1, a2, a3, b0, b1, b2, c0, c1, d0 = lax.fori_loop(0, ROWS, body, (zero,) * 10)
            x0 = a0 * cx
            xx = x0 * cx
            square = xx + a2 + c0
            terms = (a0, x0, a1, b0, square, xx, a2, a1 * cx, b0 * cx, b1, square * cx,
                     a1 * (cx * cx) + a3 + c1, b0 * (cx * cx) + b2 + d0)
            for r, term in enumerate(terms):
                acc[r] = acc[r] + term

        rank = jnp.where(positive, positives, i - positives)
        for upward in (True, False):
            @pl.when(positive if upward else jnp.logical_not(positive))
            def _(upward=upward):
                row(upward)
                for kind in range(kinds):
                    @pl.when(jnp.logical_and(rank >= offsets[kind], rank < offsets[kind + 1]))
                    def _(kind=kind):
                        target = (up if upward else down)[kind]
                        pltpu.make_async_copy(pack.at[pl.ds(i * (VB // 2), VB // 2)],
                                              target.at[pl.ds((rank - offsets[kind]) * (VB // 2), VB // 2)],
                                              out_sem.at[i]).start()
        return positives + jnp.where(positive, 1, 0)

    positives = lax.fori_loop(0, blocks, step, jnp.int32(0))
    for r in range(13):
        mom_ref[r] = acc[r] * WEIGHT
    limit = sizes[0] + sizes[1]
    excess = jnp.where(jnp.maximum(positives, blocks - positives) > limit, 1.0, 0.0)
    mom_ref[13] = jnp.full((SUB, LANES), excess, jnp.float32)

    def drain(i, carry):
        pltpu.make_async_copy(pack.at[pl.ds(i * (VB // 2), VB // 2)], up[0].at[pl.ds(0, VB // 2)], out_sem.at[i]).wait()
        return carry

    lax.fori_loop(0, blocks, drain, 0)


def gather(f, block_map, sizes):
    blocks = block_map.shape[0]
    half = VB // 2
    bufs = [jax.ShapeDtypeStruct((s * half, SUB, LANES), jnp.float32) for s in sizes if s]
    outs = pl.pallas_call(
        functools.partial(gather_kernel, sizes),
        in_specs=[pl.BlockSpec(memory_space=pltpu.SMEM), pl.BlockSpec(memory_space=pltpu.HBM)],
        out_specs=[pl.BlockSpec(memory_space=pltpu.VMEM)] + [pl.BlockSpec(memory_space=pltpu.HBM)] * (2 * len(bufs)),
        out_shape=[jax.ShapeDtypeStruct((14, SUB, LANES), jnp.float32)] + bufs + bufs,
        scratch_shapes=[pltpu.VMEM((blocks * VB, SUB, LANES), jnp.float32),
                        pltpu.VMEM((blocks * half, SUB, LANES), jnp.float32),
                        pltpu.VMEM((13, SUB, LANES), jnp.float32),
                        pltpu.SemaphoreType.DMA((blocks,)), pltpu.SemaphoreType.DMA((blocks,))],
        compiler_params=pltpu.CompilerParams(vmem_limit_bytes=VMEM_LIMIT),
        name="gather",
    )(block_map, f)
    n = len(bufs)
    return outs[0], outs[1:1 + n], outs[1 + n:]


def convert(m):
    inv = 1.0 / m[0]
    ux, uy, uz = m[1] * inv, m[2] * inv, m[3] * inv
    sq = ux * ux + uy * uy + uz * uz
    density = m[0]
    pressure = density * ((m[4] * inv - sq) / 3.0)
    xx, yy, xy, xz, yz = m[5:10]
    zz = m[4] - xx - yy
    sxx = xx - density * ux * ux - pressure
    syy = yy - density * uy * uy - pressure
    sxy = xy - density * ux * uy
    sxz = xz - density * ux * uz
    syz = yz - density * uy * uz
    hx = 0.5 * (m[10] - 2.0 * (ux * xx + uy * xy + uz * xz) - ux * m[4] + 2.0 * density * ux * sq)
    hy = 0.5 * (m[11] - 2.0 * (ux * xy + uy * yy + uz * yz) - uy * m[4] + 2.0 * density * uy * sq)
    hz = 0.5 * (m[12] - 2.0 * (ux * xz + uy * yz + uz * zz) - uz * m[4] + 2.0 * density * uz * sq)
    return [density, m[1], m[2], m[3], 0.5 * m[4]], [sxx, syy, sxy, sxz, syz, hx, hy, hz]


def primitive(state):
    density = state[0]
    inv = 1.0 / density
    ux, uy, uz = state[1] * inv, state[2] * inv, state[3] * inv
    temper = (2.0 / 3.0) * (state[4] * inv - 0.5 * (ux * ux + uy * uy + uz * uz))
    return density, ux, uy, uz, temper


def fluxes(state, extra):
    density, ux, uy, uz, temper = primitive(state)
    pressure = density * temper
    sxx, syy, sxy, sxz, syz, hx, hy, hz = extra
    szz = -sxx - syy
    enthalpy = state[4] + pressure
    fx = [state[1], state[1] * ux + pressure + sxx, state[2] * ux + sxy, state[3] * ux + sxz,
          enthalpy * ux + sxx * ux + sxy * uy + sxz * uz + hx]
    fy = [state[2], state[1] * uy + sxy, state[2] * uy + pressure + syy, state[3] * uy + syz,
          enthalpy * uy + sxy * ux + syy * uy + syz * uz + hy]
    fz = [state[3], state[1] * uz + sxz, state[2] * uz + syz, state[3] * uz + pressure + szz,
          enthalpy * uz + sxz * ux + syz * uy + szz * uz + hz]
    return fx, fy, fz


def macro_kernel(own_ref, other_ref, cross_ref, macro_ref, cell_ref):
    plane, spot, along_z = places()
    index = lax.axis_index("space")
    even = (plane * 0 + index % 2) == 0
    count = lax.axis_size("space")
    first = (plane + index) == 0
    last = (plane + (count - 1 - index)) == 3
    last = jnp.logical_and(last, plane == 3)
    states, extras = [], []
    own = [own_ref[r] for r in range(13)]
    other = [other_ref[r] for r in range(13)]
    cross = [cross_ref[r] for r in range(13)]
    low = [jnp.where(even, c, o) for c, o in zip(cross, other)]
    high = [jnp.where(even, o, c) for c, o in zip(cross, other)]
    for slab in (low, own, high):
        state, extra = convert(slab)
        states.append(state)
        extras.append(extra)

    def from_below(slabs):
        low, own, high = slabs
        a = sublane(1)(low)
        b = sublane(1)(jnp.where(plane == 3, sublane(4)(low), own))
        c = sublane(1)(jnp.where(plane == 3, sublane(4)(own), high))
        return [a, jnp.where(first, own, b), c]

    def from_above(slabs):
        low, own, high = slabs
        a = sublane(-1)(jnp.where(plane == 0, sublane(4)(own), low))
        b = sublane(-1)(jnp.where(plane == 0, sublane(4)(high), own))
        c = sublane(-1)(high)
        return [a, jnp.where(last, own, b), c]

    def y_minus(x):
        return lane(NZ)(jnp.where(spot >= LANES - NZ, sublane(4)(x), x))

    def y_plus(x):
        return lane(-NZ)(jnp.where(spot < NZ, sublane(4)(x), x))

    def z_minus(x):
        return lane(1)(jnp.where(along_z == NZ - 1, lane(-NZ)(x), x))

    def z_plus(x):
        return lane(-1)(jnp.where(along_z == 0, lane(NZ)(x), x))

    mix = DIFFUSION * MACRO_STEP
    push = 0.5 * MACRO_STEP
    for _ in range(MSTEPS):
        flux = [fluxes(s, e) for s, e in zip(states, extras)]
        fresh = [[], [], []]
        for r in range(5):
            scaled = [mix * states[k][r] for k in range(3)]
            xp = from_above([scaled[k] - push * flux[k][0][r] for k in range(3)])
            xm = from_below([scaled[k] + push * flux[k][0][r] for k in range(3)])
            for k in range(3):
                gy = push * flux[k][1][r]
                gz = push * flux[k][2][r]
                total = (1.0 - 6.0 * mix) * states[k][r] + xp[k] + xm[k]
                total = total + (y_plus(scaled[k] - gy) + y_minus(scaled[k] + gy))
                total = total + (z_plus(scaled[k] - gz) + z_minus(scaled[k] + gz))
                fresh[k].append(total)
        states = fresh
    state = states[1]
    for r in range(5):
        macro_ref[r] = state[r]
    density, ux, uy, uz, temper = primitive(state)
    logt = jnp.log(temper)
    rate = (KINETIC_STEP / VISCOSITY_REF) * density * jnp.exp((1.0 - VISCOSITY_POWER) * logt)
    skew = 1.0 / (15.0 * density * temper * temper)
    cell_ref[0] = ux
    cell_ref[1] = uy
    cell_ref[2] = uz
    cell_ref[3] = 0.5 / temper
    cell_ref[4] = rate * density * jnp.exp(-1.5 * logt)
    cell_ref[5] = extras[1][5] * skew
    cell_ref[6] = extras[1][6] * skew
    cell_ref[7] = extras[1][7] * skew
    cell_ref[8] = 1.0 - rate


def macro_solve(own, other, cross):
    vmem = pl.BlockSpec(memory_space=pltpu.VMEM)
    return pl.pallas_call(
        macro_kernel,
        in_specs=[vmem] * 3,
        out_specs=[vmem] * 2,
        out_shape=[jax.ShapeDtypeStruct((5, SUB, LANES), jnp.float32), jax.ShapeDtypeStruct((9, SUB, LANES), jnp.float32)],
        compiler_params=pltpu.CompilerParams(vmem_limit_bytes=SMALL_LIMIT),
        name="macro",
    )(own, other, cross)


def kinetic_kernel(spans, aliased, bm_ref, scal_ref, drift_ref, mask_ref, cell_ref, f_hbm, *refs):
    kinds = len(spans)
    up = refs[:kinds]
    down = refs[kinds:2 * kinds]
    refs = refs[2 * kinds + (1 if aliased else 0):]
    out_hbm, fbuf, hbuf, gz_ref, az_ref, sz_ref, iz_ref, turn_ref, yside_ref, zside_ref, pick, in_sem, halo_sem, out_sem = refs
    blocks = bm_ref.shape[0]
    low_slot = spans[0][0]
    high_slot = spans[-1][1]
    half_id = PARTS * NVX // 2
    half = VB // 2
    index = lax.axis_index("space")
    count = lax.axis_size("space")

    def choose(i, carry):
        chosen, positives = carry
        positive = bm_ref[i] >= half_id
        rank = jnp.where(positive, positives, i - positives)
        take = jnp.logical_and(rank >= low_slot, rank < high_slot)

        @pl.when(take)
        def _():
            pick[0, chosen] = i
            pick[1, chosen] = rank
        return chosen + jnp.where(take, 1, 0), positives + jnp.where(positive, 1, 0)

    chosen, _ = lax.fori_loop(0, blocks, choose, (jnp.int32(0), jnp.int32(0)))

    def fetch(n):
        i = pick[0, n]
        return pltpu.make_async_copy(f_hbm.at[pl.ds(i * VB, VB)], fbuf.at[pl.ds(i * VB, VB)], in_sem.at[i])

    def begin(n):
        fetch(n).start()
        i = pick[0, n]
        rank = pick[1, n]
        positive = bm_ref[i] >= half_id
        for upward in (True, False):
            for kind, (lo, hi) in enumerate(spans):
                here = jnp.logical_and(rank >= lo, rank < hi)

                @pl.when(jnp.logical_and(here, positive if upward else jnp.logical_not(positive)))
                def _(upward=upward, kind=kind, lo=lo):
                    source = (up if upward else down)[kind]
                    pltpu.make_async_copy(source.at[pl.ds((rank - lo) * half, half)], hbuf.at[pl.ds(i * half, half)],
                                          halo_sem.at[i]).start()

    for n in range(min(AHEAD, blocks)):
        @pl.when(n < chosen)
        def _(n=n):
            begin(n)

    plane, spot, along_z = places()
    fixed = mask_ref[...] == 1
    source = lax.broadcasted_iota(jnp.int32, (2 * LANES, LANES), 0) % LANES
    target = lax.broadcasted_iota(jnp.int32, (2 * LANES, LANES), 1)
    for step in (1, 2):
        for sign in (0, 1):
            away = step if sign else -step
            wanted_y = (target + (away * NZ + LANES)) % LANES
            wanted_z = target - target % NZ + (target % NZ + (away + NZ)) % NZ
            for which, wanted in ((sign, wanted_y), (2 + sign, wanted_z)):
                turn_ref[which, :, pl.ds((step - 1) * LANES, LANES)] = jnp.where(source == wanted, 1.0, 0.0).astype(jnp.bfloat16)
    ux, uy, uz, inv2t = cell_ref[0], cell_ref[1], cell_ref[2], cell_ref[3]
    hot = jnp.full((SUB, LANES), scal_ref[1], jnp.float32)
    hot_inv = 0.5 / hot
    hot_scale = scal_ref[0] * jnp.exp(-1.5 * jnp.log(hot))
    for e in range(NVZ):
        cz = speed(e, DZ)
        rel = cz - uz
        t = rel * rel * inv2t
        gz_ref[e] = jnp.exp(-t)
        sz_ref[e] = 2.0 * t
        az_ref[e] = rel * cell_ref[7]
        off = cz - drift_ref[2]
        iz_ref[e] = jnp.exp(-(off * off) * hot_inv)

    def run(n, carry):
        @pl.when(n + AHEAD < chosen)
        def _():
            begin(n + AHEAD)
        i = pick[0, n]
        block = bm_ref[i]
        positive = block >= half_id
        y_positive = (block % PARTS) >= PARTS // 2
        cx, cy0 = block_speeds(block)
        fetch(n).wait()
        pltpu.make_async_copy(up[0].at[pl.ds(0, half)], hbuf.at[pl.ds(i * half, half)], halo_sem.at[i]).wait()
        k0x, k1x, k2x = upwind(KINETIC_STEP * jnp.abs(cx))
        relx = cx - ux
        tx = relx * relx * inv2t
        ax = relx * cell_ref[5]
        offx = cx - drift_ref[0]

        x = fbuf[pl.ds(i * VB, VB)].reshape(VB * SUB, LANES)
        hi = x.astype(jnp.bfloat16)
        lo = (x - hi.astype(jnp.float32)).astype(jnp.bfloat16)
        both = jnp.concatenate([hi, lo], axis=1)
        yside_ref[...] = jnp.dot(both, turn_ref[jnp.where(y_positive, 0, 1)], preferred_element_type=jnp.float32)
        both = both.reshape(ROWS, 2, NVZ * SUB // 2, 2 * LANES)
        for side in (0, 1):
            part = both[:, side].reshape(VB * SUB // 2, 2 * LANES)
            zside_ref[side] = jnp.dot(part, turn_ref[3 - side], preferred_element_type=jnp.float32)

        cross1 = jnp.where(y_positive, spot, LANES - 1 - spot) < NZ
        cross2 = jnp.where(y_positive, spot, LANES - 1 - spot) < 2 * NZ

        def rows(x_up, edge):
            def one(y, carry):
                cy = cy0 + y.astype(jnp.float32) * DY
                k0y, k1y, k2y = upwind(KINETIC_STEP * jnp.abs(cy))
                rely = cy - uy
                txy = tx + rely * rely * inv2t
                axy = ax + rely * cell_ref[6]
                gxy = cell_ref[4] * jnp.exp(-txy)
                sxy = 2.0 * txy - 5.0
                keep = cell_ref[8] - (k0x + k0y)
                offy = cy - drift_ref[1]
                ixy = hot_scale * jnp.exp(-(offx * offx + offy * offy) * hot_inv)
                for e in range(NVZ):
                    k0z, k1z, k2z = upwind(KINETIC_STEP * abs(speed(e, DZ)))
                    spot_v = i * VB + y * NVZ + e
                    f = fbuf[spot_v]
                    inflow = ixy * iz_ref[e]
                    total = f * (keep - k0z)
                    if edge and x_up:
                        halo = inflow
                    elif not edge:
                        halo = hbuf[i * half + y * (NVZ // 2) + e % (NVZ // 2)]
                        if e >= NVZ // 2:
                            halo = sublane(2 if x_up else -2)(halo)
                    else:
                        halo = jnp.where(plane == 0, sublane(1)(f), sublane(2)(f))
                    if x_up:
                        x1 = sublane(1)(jnp.where(plane == 3, halo, f))
                        x2 = sublane(2)(jnp.where(plane >= 2, halo, f))
                    else:
                        x1 = sublane(-1)(jnp.where(plane == 0, halo, f))
                        x2 = sublane(-2)(jnp.where(plane < 2, halo, f))
                    total = total - k1x * x1 - k2x * x2
                    lines = pl.ds((y * NVZ + e) * SUB, SUB)
                    y1 = yside_ref[lines, :LANES]
                    y2 = yside_ref[lines, LANES:]
                    lines = pl.ds((y * (NVZ // 2) + e % (NVZ // 2)) * SUB, SUB)
                    z1 = zside_ref[e // (NVZ // 2), lines, :LANES]
                    z2 = zside_ref[e // (NVZ // 2), lines, LANES:]
                    y1 = jnp.where(cross1, sublane(4)(y1), y1)
                    y2 = jnp.where(cross2, sublane(4)(y2), y2)
                    total = total - k1y * y1 - k2y * y2
                    total = total - k1z * z1 - k2z * z2
                    shape = 1.0 + (axy + az_ref[e]) * (sxy + sz_ref[e])
                    total = total + (gxy * gz_ref[e]) * shape
                    fbuf[spot_v] = jnp.where(fixed, inflow, total)
                return carry

            lax.fori_loop(0, ROWS, one, 0)

        for x_up in (True, False):
            outer = (index == 0) if x_up else (index == count - 1)
            for edge in (True, False):
                flag = jnp.logical_and(positive if x_up else jnp.logical_not(positive),
                                       outer if edge else jnp.logical_not(outer))

                @pl.when(flag)
                def _(x_up=x_up, edge=edge):
                    rows(x_up, edge)
        pltpu.make_async_copy(fbuf.at[pl.ds(i * VB, VB)], out_hbm.at[pl.ds(i * VB, VB)], out_sem.at[i]).start()
        return carry

    lax.fori_loop(0, chosen, run, 0)

    def drain(n, carry):
        i = pick[0, n]
        pltpu.make_async_copy(fbuf.at[pl.ds(i * VB, VB)], out_hbm.at[pl.ds(i * VB, VB)], out_sem.at[i]).wait()
        return carry

    lax.fori_loop(0, chosen, drain, 0)


def kinetic(f, block_map, scalars, drift, mask, cells, spans, up, down, into=None):
    blocks = block_map.shape[0]
    half = VB // 2
    smem = pl.BlockSpec(memory_space=pltpu.SMEM)
    vmem = pl.BlockSpec(memory_space=pltpu.VMEM)
    hbm = pl.BlockSpec(memory_space=pltpu.HBM)
    operands = [block_map, scalars, drift, mask, cells, f, *up, *down]
    specs = [smem, smem, smem, vmem, vmem, hbm] + [hbm] * (len(up) + len(down))
    aliases = {}
    if into is not None:
        aliases = {len(operands): 0}
        operands.append(into)
        specs.append(hbm)
    table = pltpu.VMEM((NVZ, SUB, LANES), jnp.float32)
    return pl.pallas_call(
        functools.partial(kinetic_kernel, spans, into is not None),
        in_specs=specs,
        out_specs=hbm,
        out_shape=jax.ShapeDtypeStruct(f.shape, jnp.float32),
        scratch_shapes=[pltpu.VMEM((blocks * VB, SUB, LANES), jnp.float32), pltpu.VMEM((blocks * half, SUB, LANES), jnp.float32),
                        table, table, table, table, pltpu.VMEM((4, 2 * LANES, 2 * LANES), jnp.bfloat16),
                        pltpu.VMEM((VB * SUB, 2 * LANES), jnp.float32), pltpu.VMEM((2, VB * SUB // 2, 2 * LANES), jnp.float32),
                        pltpu.SMEM((2, blocks), jnp.int32),
                        pltpu.SemaphoreType.DMA((blocks,)), pltpu.SemaphoreType.DMA((blocks,)), pltpu.SemaphoreType.DMA((blocks,))],
        input_output_aliases=aliases,
        compiler_params=pltpu.CompilerParams(vmem_limit_bytes=VMEM_LIMIT),
        name="kinetic",
    )(*operands)


def over_vel(values):
    count = lax.axis_size("vel")
    if count & (count - 1):
        return lax.psum(values, "vel")
    reach = 1
    while reach < count:
        values = values + lax.ppermute(values, "vel", [(i, i ^ reach) for i in range(count)])
        reach *= 2
    return values


def tiles(array):
    lead, planes, width = array.shape
    return array.reshape(lead, planes, width // LANES, LANES).transpose(0, 2, 1, 3).reshape(lead, planes * width // LANES, LANES)


def per_device(distribution, block_map, inflow_mask, owner_map, inflow_scalars, inflow_drift):
    vel_count = lax.axis_size("vel")
    vel_index = lax.axis_index("vel")
    space_count = lax.axis_size("space")
    local_vel, planes, width = distribution.shape
    assert planes == MSTEPS and planes * width == SUB * LANES
    block_len = planes * width // vel_count
    blocks = block_map.shape[0]
    sizes = slot_sizes(blocks)
    f = tiles(distribution)
    mask = tiles(inflow_mask[None])[0]
    rise = [(i, i + 1) for i in range(space_count - 1)]
    fall = [(i + 1, i) for i in range(space_count - 1)]

    partial, ups, downs = gather(f, block_map, sizes)
    got_up = [lax.ppermute(ups[0], "space", rise)]
    got_down = [lax.ppermute(downs[0], "space", fall)]
    total = over_vel(partial)
    other = lax.ppermute(total, "space", [(i, i ^ 1) for i in range(space_count)])
    cross = lax.ppermute(other, "space", [(i, i + 2) for i in range(0, space_count - 2, 2)]
                         + [(i, i - 2) for i in range(3, space_count, 2)])
    if sizes[1]:
        cross, up_next, down_next = lax.optimization_barrier((cross, ups[1], downs[1]))
        got_up.append(lax.ppermute(up_next, "space", rise))
        got_down.append(lax.ppermute(down_next, "space", fall))
    macro, cells = macro_solve(total, other, cross)
    common = (f, block_map, inflow_scalars, inflow_drift, mask, cells)
    updated = kinetic(*common, ((0, sizes[0]),), got_up[:1], got_down[:1])
    if sizes[1]:
        edge = sizes[0] + sizes[1]
        spans = ((sizes[0], edge),)
        if sizes[2]:
            spans = spans + ((edge, blocks),)
            extra = lax.cond(total[13, 0, 0] > 0.5,
                             lambda a, b: (lax.ppermute(a, "space", rise), lax.ppermute(b, "space", fall)),
                             lambda a, b: (a, b), ups[2], downs[2])
            got_up.append(extra[0])
            got_down.append(extra[1])
        updated = kinetic(*common, spans, got_up[1:], got_down[1:], into=updated)
    current = updated.reshape(local_vel, width // LANES, planes, LANES).transpose(0, 2, 1, 3).reshape(local_vel, planes, width)
    flat = macro.reshape(5, width // LANES, planes, LANES).transpose(0, 2, 1, 3).reshape(5, vel_count, block_len)
    mine = lax.dynamic_slice_in_dim(flat, owner_map[vel_index], 1, axis=1).reshape(5, block_len)
    return (current, mine)


def solution(mesh):
    return jax.shard_map(
        per_device,
        mesh=mesh,
        in_specs=(P("vel", "space", None), P("vel"), P("space", None), P(), P(), P()),
        out_specs=(P("vel", "space", None), P(None, ("space", "vel"))),
        check_vma=False,
    )
```

```python
import functools
import math

import jax
import jax.numpy as jnp
from jax import lax
from jax.experimental import pallas as pl
from jax.experimental.pallas import tpu as pltpu
from jax.sharding import PartitionSpec as P

NVX = 32
NVY = 32
NVZ = 16
VB = 128
NZ = 16
MSTEPS = 4

SPEED_LIMIT = 3.5
KINETIC_STEP = 0.12
VISCOSITY_REF = 0.25
VISCOSITY_POWER = 0.81
MACRO_STEP = 0.1
DIFFUSION = 1.6

DX = 2.0 * SPEED_LIMIT / NVX
DY = 2.0 * SPEED_LIMIT / NVY
DZ = 2.0 * SPEED_LIMIT / NVZ
WEIGHT = DX * DY * DZ / (2.0 * math.pi) ** 1.5
ROWS = VB // NVZ
PARTS = NVY // ROWS
SUB = 8
LANES = 128
VMEM_LIMIT = 67_000_000
SMALL_LIMIT = 16 << 20
KINETIC_LIMIT = 24 << 20
AHEAD = 16


def speed(index, spacing):
    return -SPEED_LIMIT + (index + 0.5) * spacing


def upwind(courant):
    return 1.5 * courant - 0.5 * courant * courant, courant * courant - 2.0 * courant, 0.5 * courant - 0.5 * courant * courant


def slot_sizes(blocks):
    first = max(1, 3 * blocks // 4)
    return first, blocks - first


def block_speeds(block):
    along_x = (block // PARTS).astype(jnp.float32)
    base_y = ((block % PARTS) * ROWS).astype(jnp.float32)
    return speed(along_x, DX), speed(base_y, DY)


def sublane(shift):
    return lambda x: pltpu.roll(x, shift % SUB, 0)


def lane(shift):
    return lambda x: pltpu.roll(x, shift % LANES, 1)


def places():
    plane = lax.broadcasted_iota(jnp.int32, (SUB, LANES), 0) % 4
    spot = lax.broadcasted_iota(jnp.int32, (SUB, LANES), 1)
    return plane, spot, spot % NZ


def in_hbm(array):
    return pltpu.with_memory_space_constraint(array, pltpu.HBM)


def gather_kernel(sizes, bm_ref, f_hbm, mom_ref, *refs):
    kinds = sum(1 for s in sizes if s)
    up = refs[:kinds]
    down = refs[kinds:2 * kinds]
    fbuf, pack, acc, in_sem, out_sem = refs[2 * kinds:]
    blocks = bm_ref.shape[0]
    plane, _, _ = places()
    high = plane >= 2
    half = PARTS * NVX // 2
    offsets = [0]
    for s in sizes[:kinds]:
        offsets.append(offsets[-1] + s)

    def fetch(i):
        return pltpu.make_async_copy(f_hbm.at[pl.ds(i * VB, VB)], fbuf.at[pl.ds(i * VB, VB)], in_sem.at[i])

    for i in range(min(AHEAD, blocks)):
        fetch(i).start()
    for r in range(13):
        acc[r] = jnp.zeros((SUB, LANES), jnp.float32)

    def step(i, positives):
        @pl.when(i + AHEAD < blocks)
        def _():
            fetch(i + AHEAD).start()
        fetch(i).wait()
        block = bm_ref[i]
        positive = block >= half
        cx, cy0 = block_speeds(block)

        def row(upward):
            def body(y, carry):
                cy = cy0 + y.astype(jnp.float32) * DY
                s0 = s1 = s2 = s3 = None
                for e in range(NVZ // 2):
                    a = fbuf[i * VB + y * NVZ + e]
                    b = fbuf[i * VB + y * NVZ + e + NVZ // 2]
                    if upward:
                        pack[i * (VB // 2) + y * (NVZ // 2) + e] = jnp.where(high, sublane(4)(a), sublane(2)(b))
                    else:
                        pack[i * (VB // 2) + y * (NVZ // 2) + e] = jnp.where(high, sublane(6)(b), sublane(4)(a))
                for e in range(NVZ // 2, NVZ):
                    z = speed(e, DZ)
                    a = fbuf[i * VB + y * NVZ + e]
                    b = fbuf[i * VB + y * NVZ + NVZ - 1 - e]
                    p = a + b
                    m = (a - b) * z
                    if s0 is None:
                        s0, s1, s2, s3 = p, m, p * (z * z), m * (z * z)
                    else:
                        s0, s1, s2, s3 = s0 + p, s1 + m, s2 + p * (z * z), s3 + m * (z * z)
                a0, a1, a2, a3, b0, b1, b2, c0, c1, d0 = carry
                t1 = s0 * cy
                t2 = t1 * cy
                u1 = s1 * cy
                return (a0 + s0, a1 + t1, a2 + t2, a3 + t2 * cy, b0 + s1, b1 + u1, b2 + u1 * cy, c0 + s2, c1 + s2 * cy, d0 + s3)

            zero = jnp.zeros((SUB, LANES), jnp.float32)
            a0, a1, a2, a3, b0, b1, b2, c0, c1, d0 = lax.fori_loop(0, ROWS, body, (zero,) * 10)
            x0 = a0 * cx
            xx = x0 * cx
            square = xx + a2 + c0
            terms = (a0, x0, a1, b0, square, xx, a2, a1 * cx, b0 * cx, b1, square * cx,
                     a1 * (cx * cx) + a3 + c1, b0 * (cx * cx) + b2 + d0)
            for r, term in enumerate(terms):
                acc[r] = acc[r] + term

        rank = jnp.where(positive, positives, i - positives)
        for upward in (True, False):
            @pl.when(positive if upward else jnp.logical_not(positive))
            def _(upward=upward):
                row(upward)
                for kind in range(kinds):
                    @pl.when(jnp.logical_and(rank >= offsets[kind], rank < offsets[kind + 1]))
                    def _(kind=kind):
                        target = (up if upward else down)[kind]
                        pltpu.make_async_copy(pack.at[pl.ds(i * (VB // 2), VB // 2)],
                                              target.at[pl.ds((rank - offsets[kind]) * (VB // 2), VB // 2)],
                                              out_sem.at[i]).start()
        return positives + jnp.where(positive, 1, 0)

    positives = lax.fori_loop(0, blocks, step, jnp.int32(0))
    for r in range(13):
        mom_ref[r] = acc[r] * WEIGHT
    limit = sizes[0]
    excess = jnp.where(jnp.maximum(positives, blocks - positives) > limit, 1.0, 0.0)
    mom_ref[13] = jnp.full((SUB, LANES), excess, jnp.float32)

    def drain(i, carry):
        pltpu.make_async_copy(pack.at[pl.ds(i * (VB // 2), VB // 2)], up[0].at[pl.ds(0, VB // 2)], out_sem.at[i]).wait()
        return carry

    lax.fori_loop(0, blocks, drain, 0)


def gather(f, block_map, sizes):
    blocks = block_map.shape[0]
    half = VB // 2
    bufs = [pltpu.HBM((s * half, SUB, LANES), jnp.float32) for s in sizes if s]
    outs = pl.pallas_call(
        functools.partial(gather_kernel, sizes),
        in_specs=[pl.BlockSpec(memory_space=pltpu.SMEM), pl.BlockSpec(memory_space=pltpu.HBM)],
        out_specs=[pl.BlockSpec(memory_space=pltpu.VMEM)] + [pl.BlockSpec(memory_space=pltpu.HBM)] * (2 * len(bufs)),
        out_shape=[jax.ShapeDtypeStruct((14, SUB, LANES), jnp.float32)] + bufs + bufs,
        scratch_shapes=[pltpu.VMEM((blocks * VB, SUB, LANES), jnp.float32),
                        pltpu.VMEM((blocks * half, SUB, LANES), jnp.float32),
                        pltpu.VMEM((13, SUB, LANES), jnp.float32),
                        pltpu.SemaphoreType.DMA((blocks,)), pltpu.SemaphoreType.DMA((blocks,))],
        compiler_params=pltpu.CompilerParams(vmem_limit_bytes=VMEM_LIMIT),
        name="gather",
    )(block_map, in_hbm(f))
    n = len(bufs)
    return outs[0], outs[1:1 + n], outs[1 + n:]


def convert(m):
    inv = 1.0 / m[0]
    ux, uy, uz = m[1] * inv, m[2] * inv, m[3] * inv
    sq = ux * ux + uy * uy + uz * uz
    density = m[0]
    pressure = density * ((m[4] * inv - sq) / 3.0)
    xx, yy, xy, xz, yz = m[5:10]
    zz = m[4] - xx - yy
    sxx = xx - density * ux * ux - pressure
    syy = yy - density * uy * uy - pressure
    sxy = xy - density * ux * uy
    sxz = xz - density * ux * uz
    syz = yz - density * uy * uz
    hx = 0.5 * (m[10] - 2.0 * (ux * xx + uy * xy + uz * xz) - ux * m[4] + 2.0 * density * ux * sq)
    hy = 0.5 * (m[11] - 2.0 * (ux * xy + uy * yy + uz * yz) - uy * m[4] + 2.0 * density * uy * sq)
    hz = 0.5 * (m[12] - 2.0 * (ux * xz + uy * yz + uz * zz) - uz * m[4] + 2.0 * density * uz * sq)
    return [density, m[1], m[2], m[3], 0.5 * m[4]], [sxx, syy, sxy, sxz, syz, hx, hy, hz]


def primitive(state):
    density = state[0]
    inv = 1.0 / density
    ux, uy, uz = state[1] * inv, state[2] * inv, state[3] * inv
    temper = (2.0 / 3.0) * (state[4] * inv - 0.5 * (ux * ux + uy * uy + uz * uz))
    return density, ux, uy, uz, temper


def fluxes(state, extra):
    density, ux, uy, uz, temper = primitive(state)
    pressure = density * temper
    sxx, syy, sxy, sxz, syz, hx, hy, hz = extra
    szz = -sxx - syy
    enthalpy = state[4] + pressure
    fx = [state[1], state[1] * ux + pressure + sxx, state[2] * ux + sxy, state[3] * ux + sxz,
          enthalpy * ux + sxx * ux + sxy * uy + sxz * uz + hx]
    fy = [state[2], state[1] * uy + sxy, state[2] * uy + pressure + syy, state[3] * uy + syz,
          enthalpy * uy + sxy * ux + syy * uy + syz * uz + hy]
    fz = [state[3], state[1] * uz + sxz, state[2] * uz + syz, state[3] * uz + pressure + szz,
          enthalpy * uz + sxz * ux + syz * uy + szz * uz + hz]
    return fx, fy, fz


def macro_kernel(own_ref, other_ref, cross_ref, macro_ref, cell_ref):
    plane, spot, along_z = places()
    index = lax.axis_index("space")
    even = (plane * 0 + index % 2) == 0
    count = lax.axis_size("space")
    first = (plane + index) == 0
    last = (plane + (count - 1 - index)) == 3
    last = jnp.logical_and(last, plane == 3)
    states, extras = [], []
    own = [own_ref[r] for r in range(13)]
    other = [other_ref[r] for r in range(13)]
    cross = [cross_ref[r] for r in range(13)]
    low = [jnp.where(even, c, o) for c, o in zip(cross, other)]
    high = [jnp.where(even, o, c) for c, o in zip(cross, other)]
    for slab in (low, own, high):
        state, extra = convert(slab)
        states.append(state)
        extras.append(extra)

    def from_below(slabs):
        low, own, high = slabs
        a = sublane(1)(low)
        b = sublane(1)(jnp.where(plane == 3, sublane(4)(low), own))
        c = sublane(1)(jnp.where(plane == 3, sublane(4)(own), high))
        return [a, jnp.where(first, own, b), c]

    def from_above(slabs):
        low, own, high = slabs
        a = sublane(-1)(jnp.where(plane == 0, sublane(4)(own), low))
        b = sublane(-1)(jnp.where(plane == 0, sublane(4)(high), own))
        c = sublane(-1)(high)
        return [a, jnp.where(last, own, b), c]

    def y_minus(x):
        return lane(NZ)(jnp.where(spot >= LANES - NZ, sublane(4)(x), x))

    def y_plus(x):
        return lane(-NZ)(jnp.where(spot < NZ, sublane(4)(x), x))

    def z_minus(x):
        return lane(1)(jnp.where(along_z == NZ - 1, lane(-NZ)(x), x))

    def z_plus(x):
        return lane(-1)(jnp.where(along_z == 0, lane(NZ)(x), x))

    mix = DIFFUSION * MACRO_STEP
    push = 0.5 * MACRO_STEP
    for _ in range(MSTEPS):
        flux = [fluxes(s, e) for s, e in zip(states, extras)]
        fresh = [[], [], []]
        for r in range(5):
            scaled = [mix * states[k][r] for k in range(3)]
            xp = from_above([scaled[k] - push * flux[k][0][r] for k in range(3)])
            xm = from_below([scaled[k] + push * flux[k][0][r] for k in range(3)])
            for k in range(3):
                gy = push * flux[k][1][r]
                gz = push * flux[k][2][r]
                total = (1.0 - 6.0 * mix) * states[k][r] + xp[k] + xm[k]
                total = total + (y_plus(scaled[k] - gy) + y_minus(scaled[k] + gy))
                total = total + (z_plus(scaled[k] - gz) + z_minus(scaled[k] + gz))
                fresh[k].append(total)
        states = fresh
    state = states[1]
    for r in range(5):
        macro_ref[r] = state[r]
    density, ux, uy, uz, temper = primitive(state)
    logt = jnp.log(temper)
    rate = (KINETIC_STEP / VISCOSITY_REF) * density * jnp.exp((1.0 - VISCOSITY_POWER) * logt)
    skew = 1.0 / (15.0 * density * temper * temper)
    cell_ref[0] = ux
    cell_ref[1] = uy
    cell_ref[2] = uz
    cell_ref[3] = 0.5 / temper
    cell_ref[4] = rate * density * jnp.exp(-1.5 * logt)
    cell_ref[5] = extras[1][5] * skew
    cell_ref[6] = extras[1][6] * skew
    cell_ref[7] = extras[1][7] * skew
    cell_ref[8] = 1.0 - rate


def macro_solve(own, other, cross):
    vmem = pl.BlockSpec(memory_space=pltpu.VMEM)
    return pl.pallas_call(
        macro_kernel,
        in_specs=[vmem] * 3,
        out_specs=[vmem] * 2,
        out_shape=[jax.ShapeDtypeStruct((5, SUB, LANES), jnp.float32), jax.ShapeDtypeStruct((9, SUB, LANES), jnp.float32)],
        compiler_params=pltpu.CompilerParams(vmem_limit_bytes=SMALL_LIMIT),
        name="macro",
    )(own, other, cross)


def kinetic_kernel(bm_ref, scal_ref, drift_ref, mask_ref, cell_ref, f_hbm, out_ref, *refs):
    gz_ref, az_ref, sz_ref, iz_ref, turn_ref, ylow_ref, yhigh_ref, zlow_ref, zhigh_ref, in_sem = refs
    ysides, zsides = (ylow_ref, yhigh_ref), (zlow_ref, zhigh_ref)
    blocks = bm_ref.shape[0]
    half_id = PARTS * NVX // 2
    index = lax.axis_index("space")
    count = lax.axis_size("space")

    def fetch(i):
        return pltpu.make_async_copy(f_hbm.at[pl.ds(i * VB, VB)], out_ref.at[pl.ds(i * VB, VB)], in_sem.at[i])

    for i in range(blocks):
        fetch(i).start()

    plane, spot, along_z = places()
    fixed = mask_ref[...] == 1
    source = lax.broadcasted_iota(jnp.int32, (2 * LANES, LANES), 0) % LANES
    target = lax.broadcasted_iota(jnp.int32, (2 * LANES, LANES), 1)
    for step in (1, 2):
        for sign in (0, 1):
            away = step if sign else -step
            wanted_y = (target + (away * NZ + LANES)) % LANES
            wanted_z = target - target % NZ + (target % NZ + (away + NZ)) % NZ
            for which, wanted in ((sign, wanted_y), (2 + sign, wanted_z)):
                turn_ref[which, :, pl.ds((step - 1) * LANES, LANES)] = jnp.where(source == wanted, 1.0, 0.0).astype(jnp.bfloat16)
    ux, uy, uz, inv2t = cell_ref[0], cell_ref[1], cell_ref[2], cell_ref[3]
    hot = jnp.full((SUB, LANES), scal_ref[1], jnp.float32)
    hot_inv = 0.5 / hot
    hot_scale = scal_ref[0] * jnp.exp(-1.5 * jnp.log(hot))
    for e in range(NVZ):
        cz = speed(e, DZ)
        rel = cz - uz
        t = rel * rel * inv2t
        gz_ref[e] = jnp.exp(-t)
        sz_ref[e] = 2.0 * t
        az_ref[e] = rel * cell_ref[7]
        off = cz - drift_ref[2]
        iz_ref[e] = jnp.exp(-(off * off) * hot_inv)

    part_rows = ROWS // 2
    part_size = part_rows * NVZ

    def shifts(i, part):
        x = out_ref[pl.ds(i * VB + part * part_size, part_size)].reshape(part_size * SUB, LANES)
        hi = x.astype(jnp.bfloat16)
        lo = (x - hi.astype(jnp.float32)).astype(jnp.bfloat16)
        both = jnp.concatenate([hi, lo], axis=1)
        which = jnp.where((bm_ref[i] % PARTS) >= PARTS // 2, 0, 1)
        ysides[part][...] = jnp.dot(both, turn_ref[which], preferred_element_type=jnp.float32)
        both = both.reshape(part_rows, 2, NVZ * SUB // 2, 2 * LANES)
        for side in (0, 1):
            lines = both[:, side].reshape(part_size * SUB // 2, 2 * LANES)
            zsides[part][side] = jnp.dot(lines, turn_ref[3 - side], preferred_element_type=jnp.float32)

    fetch(0).wait()
    shifts(0, 0)

    def run(i, carry):
        block = bm_ref[i]
        positive = block >= half_id
        y_positive = (block % PARTS) >= PARTS // 2
        cx, cy0 = block_speeds(block)

        @pl.when(i + 1 < blocks)
        def _():
            fetch(i + 1).wait()
        following = jnp.minimum(i + 1, blocks - 1)
        k0x, k1x, k2x = upwind(KINETIC_STEP * jnp.abs(cx))
        relx = cx - ux
        tx = relx * relx * inv2t
        ax = relx * cell_ref[5]
        offx = cx - drift_ref[0]

        cross1 = jnp.where(y_positive, spot, LANES - 1 - spot) < NZ
        cross2 = jnp.where(y_positive, spot, LANES - 1 - spot) < 2 * NZ

        def rows(x_up, edge):
            def one(y):
                yside_ref, zside_ref = ysides[y // part_rows], zsides[y // part_rows]
                r = y % part_rows
                cy = cy0 + y * DY
                k0y, k1y, k2y = upwind(KINETIC_STEP * jnp.abs(cy))
                rely = cy - uy
                txy = tx + rely * rely * inv2t
                axy = ax + rely * cell_ref[6]
                gxy = cell_ref[4] * jnp.exp(-txy)
                sxy = 2.0 * txy - 5.0
                keep = cell_ref[8] - (k0x + k0y)
                offy = cy - drift_ref[1]
                ixy = hot_scale * jnp.exp(-(offx * offx + offy * offy) * hot_inv)
                for e in range(NVZ):
                    k0z, k1z, k2z = upwind(KINETIC_STEP * abs(speed(e, DZ)))
                    spot_v = i * VB + y * NVZ + e
                    f = out_ref[spot_v]
                    inflow = ixy * iz_ref[e]
                    total = f * (keep - k0z)
                    if edge and x_up:
                        halo = inflow
                    elif not edge:
                        halo = 0.0
                    else:
                        halo = jnp.where(plane == 0, sublane(1)(f), sublane(2)(f))
                    if x_up:
                        x1 = sublane(1)(jnp.where(plane == 3, halo, f))
                        x2 = sublane(2)(jnp.where(plane >= 2, halo, f))
                    else:
                        x1 = sublane(-1)(jnp.where(plane == 0, halo, f))
                        x2 = sublane(-2)(jnp.where(plane < 2, halo, f))
                    total = total - k1x * x1 - k2x * x2
                    lines = pl.ds((r * NVZ + e) * SUB, SUB)
                    y1 = yside_ref[lines, :LANES]
                    y2 = yside_ref[lines, LANES:]
                    lines = pl.ds((r * (NVZ // 2) + e % (NVZ // 2)) * SUB, SUB)
                    z1 = zside_ref[e // (NVZ // 2), lines, :LANES]
                    z2 = zside_ref[e // (NVZ // 2), lines, LANES:]
                    y1 = jnp.where(cross1, sublane(4)(y1), y1)
                    y2 = jnp.where(cross2, sublane(4)(y2), y2)
                    total = total - k1y * y1 - k2y * y2
                    total = total - k1z * z1 - k2z * z2
                    shape = 1.0 + (axy + az_ref[e]) * (sxy + sz_ref[e])
                    total = total + (gxy * gz_ref[e]) * shape
                    out_ref[spot_v] = jnp.where(fixed, inflow, total)

            shifts(i, 1)
            for y in range(part_rows):
                one(y)
            shifts(following, 0)
            for y in range(part_rows, ROWS):
                one(y)

        for x_up in (True, False):
            outer = (index == 0) if x_up else (index == count - 1)
            for edge in (True, False):
                flag = jnp.logical_and(positive if x_up else jnp.logical_not(positive),
                                       outer if edge else jnp.logical_not(outer))

                @pl.when(flag)
                def _(x_up=x_up, edge=edge):
                    rows(x_up, edge)
        return carry

    lax.fori_loop(0, blocks, run, 0)


def kinetic(f, block_map, scalars, drift, mask, cells):
    blocks = block_map.shape[0]
    smem = pl.BlockSpec(memory_space=pltpu.SMEM)
    vmem = pl.BlockSpec(memory_space=pltpu.VMEM)
    table = pltpu.VMEM((NVZ, SUB, LANES), jnp.float32)
    yside = pltpu.VMEM((VB * SUB // 2, 2 * LANES), jnp.float32)
    zside = pltpu.VMEM((2, VB * SUB // 4, 2 * LANES), jnp.float32)
    return pl.pallas_call(
        kinetic_kernel,
        in_specs=[smem, smem, smem, vmem, vmem, pl.BlockSpec(memory_space=pltpu.HBM)],
        out_specs=vmem,
        out_shape=pltpu.VMEM(f.shape, jnp.float32),
        scratch_shapes=[table, table, table, table, pltpu.VMEM((4, 2 * LANES, 2 * LANES), jnp.bfloat16),
                        yside, yside, zside, zside, pltpu.SemaphoreType.DMA((blocks,))],
        compiler_params=pltpu.CompilerParams(vmem_limit_bytes=KINETIC_LIMIT),
        name="kinetic",
    )(block_map, scalars, drift, mask, cells, in_hbm(f))


def halo_kernel(sizes, bm_ref, mask_ref, part_ref, *refs):
    kinds = sum(1 for size in sizes if size)
    up = refs[:kinds]
    down = refs[kinds:2 * kinds]
    out_hbm, obuf, late, out_sem, late_sem = refs[2 * kinds:]
    blocks = bm_ref.shape[0]
    half_id = PARTS * NVX // 2
    half = VB // 2
    index = lax.axis_index("space")
    count = lax.axis_size("space")
    plane, _, _ = places()
    fixed = mask_ref[...] == 1

    def run(i, positives):
        block = bm_ref[i]
        positive = block >= half_id
        rank = jnp.where(positive, positives, i - positives)
        cx, _ = block_speeds(block)
        _, k1x, k2x = upwind(KINETIC_STEP * jnp.abs(cx))
        outer = jnp.where(positive, index == 0, index == count - 1)

        def rows(x_up, source, base):
            if x_up:
                near, far = plane == 3, plane >= 2
            else:
                near, far = plane == 0, plane < 2
            turn = 1 if x_up else -1

            def body(y, carry):
                for e in range(NVZ // 2):
                    pair = source[base + y * (NVZ // 2) + e]
                    for side in (0, 1):
                        halo = sublane(2 * turn)(pair) if side else pair
                        spot_v = i * VB + y * NVZ + e + side * (NVZ // 2)
                        brought = sublane(turn)(jnp.where(near, halo * k1x, 0.0)) + sublane(2 * turn)(jnp.where(far, halo * k2x, 0.0))
                        old = part_ref[spot_v]
                        obuf[spot_v] = jnp.where(fixed, old, old - brought)
                return carry

            lax.fori_loop(0, ROWS, body, 0)

        @pl.when(outer)
        def _():
            def body(y, carry):
                for e in range(NVZ):
                    obuf[i * VB + y * NVZ + e] = part_ref[i * VB + y * NVZ + e]
                return carry

            lax.fori_loop(0, ROWS, body, 0)

        inner = jnp.logical_not(outer)
        for x_up in (True, False):
            mine = jnp.logical_and(inner, positive if x_up else jnp.logical_not(positive))
            source = up if x_up else down

            @pl.when(jnp.logical_and(mine, rank < sizes[0]))
            def _(x_up=x_up, source=source):
                rows(x_up, source[0], rank * half)

            if kinds > 1:
                @pl.when(jnp.logical_and(mine, rank >= sizes[0]))
                def _(x_up=x_up, source=source):
                    copy = pltpu.make_async_copy(source[1].at[pl.ds((rank - sizes[0]) * half, half)], late, late_sem)
                    copy.start()
                    copy.wait()
                    rows(x_up, late, 0)
        pltpu.make_async_copy(obuf.at[pl.ds(i * VB, VB)], out_hbm.at[pl.ds(i * VB, VB)], out_sem.at[i]).start()
        return positives + jnp.where(positive, 1, 0)

    lax.fori_loop(0, blocks, run, jnp.int32(0))

    def drain(i, carry):
        pltpu.make_async_copy(obuf.at[pl.ds(i * VB, VB)], out_hbm.at[pl.ds(i * VB, VB)], out_sem.at[i]).wait()
        return carry

    lax.fori_loop(0, blocks, drain, 0)


def halo_update(part, block_map, mask, sizes, up, down):
    blocks = block_map.shape[0]
    smem = pl.BlockSpec(memory_space=pltpu.SMEM)
    vmem = pl.BlockSpec(memory_space=pltpu.VMEM)
    hbm = pl.BlockSpec(memory_space=pltpu.HBM)
    places_of = ([vmem] + [hbm] * (len(up) - 1)) * 2
    return pl.pallas_call(
        functools.partial(halo_kernel, sizes),
        in_specs=[smem, vmem, vmem] + places_of,
        out_specs=hbm,
        out_shape=jax.ShapeDtypeStruct(part.shape, jnp.float32),
        scratch_shapes=[pltpu.VMEM((blocks * VB, SUB, LANES), jnp.float32), pltpu.VMEM((VB // 2, SUB, LANES), jnp.float32),
                        pltpu.SemaphoreType.DMA((blocks,)), pltpu.SemaphoreType.DMA],
        compiler_params=pltpu.CompilerParams(vmem_limit_bytes=KINETIC_LIMIT),
        name="halo",
    )(block_map, mask, part, up[0], *map(in_hbm, up[1:]), down[0], *map(in_hbm, down[1:]))


def over_vel(values):
    count = lax.axis_size("vel")
    if count & (count - 1):
        return lax.psum(values, "vel")
    reach = 1
    while reach < count:
        values = values + lax.ppermute(values, "vel", [(i, i ^ reach) for i in range(count)])
        reach *= 2
    return values


def tiles(array):
    lead, planes, width = array.shape
    return array.reshape(lead, planes, width // LANES, LANES).transpose(0, 2, 1, 3).reshape(lead, planes * width // LANES, LANES)


def per_device(distribution, block_map, inflow_mask, owner_map, inflow_scalars, inflow_drift):
    vel_count = lax.axis_size("vel")
    vel_index = lax.axis_index("vel")
    space_count = lax.axis_size("space")
    local_vel, planes, width = distribution.shape
    assert planes == MSTEPS and planes * width == SUB * LANES
    block_len = planes * width // vel_count
    blocks = block_map.shape[0]
    sizes = slot_sizes(blocks)
    f = tiles(distribution)
    mask = tiles(inflow_mask[None])[0]
    rise = [(i, i + 1) for i in range(space_count - 1)]
    fall = [(i + 1, i) for i in range(space_count - 1)]

    partial, ups, downs = gather(f, block_map, sizes)
    got_up = [lax.ppermute(ups[0], "space", rise)]
    got_down = [lax.ppermute(downs[0], "space", fall)]
    total = over_vel(partial)
    other = lax.ppermute(total, "space", [(i, i ^ 1) for i in range(space_count)])
    cross = lax.ppermute(other, "space", [(i, i + 2) for i in range(0, space_count - 2, 2)]
                         + [(i, i - 2) for i in range(3, space_count, 2)])
    macro, cells = macro_solve(total, other, cross)
    part = kinetic(f, block_map, inflow_scalars, inflow_drift, mask, cells)
    if sizes[1]:
        extra = lax.cond(total[13, 0, 0] > 0.5,
                         lambda a, b: (lax.ppermute(a, "space", rise), lax.ppermute(b, "space", fall)),
                         lambda a, b: (a, b), ups[1], downs[1])
        got_up.append(extra[0])
        got_down.append(extra[1])
    updated = halo_update(part, block_map, mask, sizes, got_up, got_down)
    current = updated.reshape(local_vel, width // LANES, planes, LANES).transpose(0, 2, 1, 3).reshape(local_vel, planes, width)
    flat = macro.reshape(5, width // LANES, planes, LANES).transpose(0, 2, 1, 3).reshape(5, vel_count, block_len)
    mine = lax.dynamic_slice_in_dim(flat, owner_map[vel_index], 1, axis=1).reshape(5, block_len)
    return (current, mine)


def solution(mesh):
    return jax.shard_map(
        per_device,
        mesh=mesh,
        in_specs=(P("vel", "space", None), P("vel"), P("space", None), P(), P(), P()),
        out_specs=(P("vel", "space", None), P(None, ("space", "vel"))),
        check_vma=False,
    )
```

```python
import functools
import math

import jax
import jax.numpy as jnp
from jax import lax
from jax.experimental import pallas as pl
from jax.experimental.pallas import tpu as pltpu
from jax.sharding import PartitionSpec as P

NVX = 32
NVY = 32
NVZ = 16
VB = 128
NZ = 16
MSTEPS = 4

SPEED_LIMIT = 3.5
KINETIC_STEP = 0.12
VISCOSITY_REF = 0.25
VISCOSITY_POWER = 0.81
MACRO_STEP = 0.1
DIFFUSION = 1.6

DX = 2.0 * SPEED_LIMIT / NVX
DY = 2.0 * SPEED_LIMIT / NVY
DZ = 2.0 * SPEED_LIMIT / NVZ
WEIGHT = DX * DY * DZ / (2.0 * math.pi) ** 1.5
ROWS = VB // NVZ
PARTS = NVY // ROWS
SUB = 8
LANES = 128
SMALL_LIMIT = 16 << 20
KINETIC_LIMIT = 24 << 20
AHEAD = 16


def speed(index, spacing):
    return -SPEED_LIMIT + (index + 0.5) * spacing


def upwind(courant):
    return 1.5 * courant - 0.5 * courant * courant, courant * courant - 2.0 * courant, 0.5 * courant - 0.5 * courant * courant


def slot_sizes(blocks):
    first = max(1, 3 * blocks // 4)
    return first, blocks - first


def block_speeds(block):
    along_x = (block // PARTS).astype(jnp.float32)
    base_y = ((block % PARTS) * ROWS).astype(jnp.float32)
    return speed(along_x, DX), speed(base_y, DY)


def sublane(shift):
    return lambda x: pltpu.roll(x, shift % SUB, 0)


def lane(shift):
    return lambda x: pltpu.roll(x, shift % LANES, 1)


def places():
    plane = lax.broadcasted_iota(jnp.int32, (SUB, LANES), 0) % 4
    spot = lax.broadcasted_iota(jnp.int32, (SUB, LANES), 1)
    return plane, spot, spot % NZ


def in_hbm(array):
    return pltpu.with_memory_space_constraint(array, pltpu.HBM)


def in_vmem(array):
    return pltpu.with_memory_space_constraint(array, pltpu.VMEM)


def gather_kernel(sizes, bm_ref, f_hbm, mom_ref, *refs):
    kinds = sum(1 for s in sizes if s)
    up = refs[:kinds]
    down = refs[kinds:2 * kinds]
    fbuf, pack, acc, in_sem, out_sem = refs[2 * kinds:]
    blocks = bm_ref.shape[0]
    plane, _, _ = places()
    high = plane >= 2
    half = PARTS * NVX // 2
    offsets = [0]
    for s in sizes[:kinds]:
        offsets.append(offsets[-1] + s)

    def fetch(i):
        return pltpu.make_async_copy(f_hbm.at[pl.ds(i * VB, VB)], fbuf.at[pl.ds(i * VB, VB)], in_sem.at[i])

    for i in range(min(AHEAD, blocks)):
        fetch(i).start()
    for r in range(13):
        acc[r] = jnp.zeros((SUB, LANES), jnp.float32)

    def step(i, positives):
        @pl.when(i + AHEAD < blocks)
        def _():
            fetch(i + AHEAD).start()
        fetch(i).wait()
        block = bm_ref[i]
        positive = block >= half
        cx, cy0 = block_speeds(block)

        def row(upward):
            def body(y, carry):
                cy = cy0 + y.astype(jnp.float32) * DY
                s0 = s1 = s2 = s3 = None
                for e in range(NVZ // 2):
                    a = fbuf[i * VB + y * NVZ + e]
                    b = fbuf[i * VB + y * NVZ + e + NVZ // 2]
                    if upward:
                        pack[i * (VB // 2) + y * (NVZ // 2) + e] = jnp.where(high, sublane(4)(a), sublane(2)(b))
                    else:
                        pack[i * (VB // 2) + y * (NVZ // 2) + e] = jnp.where(high, sublane(6)(b), sublane(4)(a))
                for e in range(NVZ // 2, NVZ):
                    z = speed(e, DZ)
                    a = fbuf[i * VB + y * NVZ + e]
                    b = fbuf[i * VB + y * NVZ + NVZ - 1 - e]
                    p = a + b
                    m = (a - b) * z
                    if s0 is None:
                        s0, s1, s2, s3 = p, m, p * (z * z), m * (z * z)
                    else:
                        s0, s1, s2, s3 = s0 + p, s1 + m, s2 + p * (z * z), s3 + m * (z * z)
                a0, a1, a2, a3, b0, b1, b2, c0, c1, d0 = carry
                t1 = s0 * cy
                t2 = t1 * cy
                u1 = s1 * cy
                return (a0 + s0, a1 + t1, a2 + t2, a3 + t2 * cy, b0 + s1, b1 + u1, b2 + u1 * cy, c0 + s2, c1 + s2 * cy, d0 + s3)

            zero = jnp.zeros((SUB, LANES), jnp.float32)
            a0, a1, a2, a3, b0, b1, b2, c0, c1, d0 = lax.fori_loop(0, ROWS, body, (zero,) * 10)
            x0 = a0 * cx
            xx = x0 * cx
            square = xx + a2 + c0
            terms = (a0, x0, a1, b0, square, xx, a2, a1 * cx, b0 * cx, b1, square * cx,
                     a1 * (cx * cx) + a3 + c1, b0 * (cx * cx) + b2 + d0)
            for r, term in enumerate(terms):
                acc[r] = acc[r] + term

        rank = jnp.where(positive, positives, i - positives)
        for upward in (True, False):
            @pl.when(positive if upward else jnp.logical_not(positive))
            def _(upward=upward):
                row(upward)
                for kind in range(kinds):
                    @pl.when(jnp.logical_and(rank >= offsets[kind], rank < offsets[kind + 1]))
                    def _(kind=kind):
                        target = (up if upward else down)[kind]
                        pltpu.make_async_copy(pack.at[pl.ds(i * (VB // 2), VB // 2)],
                                              target.at[pl.ds((rank - offsets[kind]) * (VB // 2), VB // 2)],
                                              out_sem.at[i]).start()
        return positives + jnp.where(positive, 1, 0)

    positives = lax.fori_loop(0, blocks, step, jnp.int32(0))
    for r in range(13):
        mom_ref[r] = acc[r] * WEIGHT
    limit = sizes[0]
    excess = jnp.where(jnp.maximum(positives, blocks - positives) > limit, 1.0, 0.0)
    mom_ref[13] = jnp.full((SUB, LANES), excess, jnp.float32)

    def drain(i, carry):
        pltpu.make_async_copy(pack.at[pl.ds(i * (VB // 2), VB // 2)], up[0].at[pl.ds(0, VB // 2)], out_sem.at[i]).wait()
        return carry

    lax.fori_loop(0, blocks, drain, 0)


def gather(f, block_map, sizes):
    blocks = block_map.shape[0]
    half = VB // 2
    bufs = [pltpu.HBM((s * half, SUB, LANES), jnp.float32) for s in sizes if s]
    outs = pl.pallas_call(
        functools.partial(gather_kernel, sizes),
        in_specs=[pl.BlockSpec(memory_space=pltpu.SMEM), pl.BlockSpec(memory_space=pltpu.HBM)],
        out_specs=[pl.BlockSpec(memory_space=pltpu.VMEM)] + [pl.BlockSpec(memory_space=pltpu.HBM)] * (2 * len(bufs)),
        out_shape=[pltpu.VMEM((14, SUB, LANES), jnp.float32)] + bufs + bufs,
        scratch_shapes=[pltpu.VMEM(f.shape, jnp.float32), pltpu.VMEM((blocks * half, SUB, LANES), jnp.float32),
                        pltpu.VMEM((13, SUB, LANES), jnp.float32),
                        pltpu.SemaphoreType.DMA((blocks,)), pltpu.SemaphoreType.DMA((blocks,))],
        compiler_params=pltpu.CompilerParams(vmem_limit_bytes=KINETIC_LIMIT),
        name="gather",
    )(block_map, in_hbm(f))
    n = len(bufs)
    return outs[0], outs[1:1 + n], outs[1 + n:]


def convert(m):
    inv = 1.0 / m[0]
    ux, uy, uz = m[1] * inv, m[2] * inv, m[3] * inv
    sq = ux * ux + uy * uy + uz * uz
    density = m[0]
    pressure = density * ((m[4] * inv - sq) / 3.0)
    xx, yy, xy, xz, yz = m[5:10]
    zz = m[4] - xx - yy
    sxx = xx - density * ux * ux - pressure
    syy = yy - density * uy * uy - pressure
    sxy = xy - density * ux * uy
    sxz = xz - density * ux * uz
    syz = yz - density * uy * uz
    hx = 0.5 * (m[10] - 2.0 * (ux * xx + uy * xy + uz * xz) - ux * m[4] + 2.0 * density * ux * sq)
    hy = 0.5 * (m[11] - 2.0 * (ux * xy + uy * yy + uz * yz) - uy * m[4] + 2.0 * density * uy * sq)
    hz = 0.5 * (m[12] - 2.0 * (ux * xz + uy * yz + uz * zz) - uz * m[4] + 2.0 * density * uz * sq)
    return [density, m[1], m[2], m[3], 0.5 * m[4]], [sxx, syy, sxy, sxz, syz, hx, hy, hz]


def primitive(state):
    density = state[0]
    inv = 1.0 / density
    ux, uy, uz = state[1] * inv, state[2] * inv, state[3] * inv
    temper = (2.0 / 3.0) * (state[4] * inv - 0.5 * (ux * ux + uy * uy + uz * uz))
    return density, ux, uy, uz, temper


def fluxes(state, extra):
    density, ux, uy, uz, temper = primitive(state)
    pressure = density * temper
    sxx, syy, sxy, sxz, syz, hx, hy, hz = extra
    szz = -sxx - syy
    enthalpy = state[4] + pressure
    fx = [state[1], state[1] * ux + pressure + sxx, state[2] * ux + sxy, state[3] * ux + sxz,
          enthalpy * ux + sxx * ux + sxy * uy + sxz * uz + hx]
    fy = [state[2], state[1] * uy + sxy, state[2] * uy + pressure + syy, state[3] * uy + syz,
          enthalpy * uy + sxy * ux + syy * uy + syz * uz + hy]
    fz = [state[3], state[1] * uz + sxz, state[2] * uz + syz, state[3] * uz + pressure + szz,
          enthalpy * uz + sxz * ux + syz * uy + szz * uz + hz]
    return fx, fy, fz


def macro_kernel(owner_ref, own_ref, other_ref, cross_ref, macro_ref, cell_ref, mine_ref, flag_ref):
    plane, spot, along_z = places()
    index = lax.axis_index("space")
    even = (plane * 0 + index % 2) == 0
    count = lax.axis_size("space")
    first = (plane + index) == 0
    last = (plane + (count - 1 - index)) == 3
    last = jnp.logical_and(last, plane == 3)
    states, extras = [], []
    own = [own_ref[r] for r in range(13)]
    other = [other_ref[r] for r in range(13)]
    cross = [cross_ref[r] for r in range(13)]
    low = [jnp.where(even, c, o) for c, o in zip(cross, other)]
    high = [jnp.where(even, o, c) for c, o in zip(cross, other)]
    for slab in (low, own, high):
        state, extra = convert(slab)
        states.append(state)
        extras.append(extra)

    def from_below(slabs):
        low, own, high = slabs
        a = sublane(1)(low)
        b = sublane(1)(jnp.where(plane == 3, sublane(4)(low), own))
        c = sublane(1)(jnp.where(plane == 3, sublane(4)(own), high))
        return [a, jnp.where(first, own, b), c]

    def from_above(slabs):
        low, own, high = slabs
        a = sublane(-1)(jnp.where(plane == 0, sublane(4)(own), low))
        b = sublane(-1)(jnp.where(plane == 0, sublane(4)(high), own))
        c = sublane(-1)(high)
        return [a, jnp.where(last, own, b), c]

    def y_minus(x):
        return lane(NZ)(jnp.where(spot >= LANES - NZ, sublane(4)(x), x))

    def y_plus(x):
        return lane(-NZ)(jnp.where(spot < NZ, sublane(4)(x), x))

    def z_minus(x):
        return lane(1)(jnp.where(along_z == NZ - 1, lane(-NZ)(x), x))

    def z_plus(x):
        return lane(-1)(jnp.where(along_z == 0, lane(NZ)(x), x))

    mix = DIFFUSION * MACRO_STEP
    push = 0.5 * MACRO_STEP
    for _ in range(MSTEPS):
        flux = [fluxes(s, e) for s, e in zip(states, extras)]
        fresh = [[], [], []]
        for r in range(5):
            scaled = [mix * states[k][r] for k in range(3)]
            xp = from_above([scaled[k] - push * flux[k][0][r] for k in range(3)])
            xm = from_below([scaled[k] + push * flux[k][0][r] for k in range(3)])
            for k in range(3):
                gy = push * flux[k][1][r]
                gz = push * flux[k][2][r]
                total = (1.0 - 6.0 * mix) * states[k][r] + xp[k] + xm[k]
                total = total + (y_plus(scaled[k] - gy) + y_minus(scaled[k] + gy))
                total = total + (z_plus(scaled[k] - gz) + z_minus(scaled[k] + gz))
                fresh[k].append(total)
        states = fresh
    state = states[1]
    for r in range(5):
        macro_ref[r] = state[r]
    row = owner_ref[lax.axis_index("vel")] % SUB
    here = (row % 2) * 4 + row // 2
    for r in range(5):
        mine_ref[pl.ds(r, 1), :] = macro_ref[r, pl.ds(here, 1), :]
    flag_ref[0] = jnp.where(jnp.max(own_ref[13]) > 0.5, 1, 0)
    density, ux, uy, uz, temper = primitive(state)
    logt = jnp.log(temper)
    rate = (KINETIC_STEP / VISCOSITY_REF) * density * jnp.exp((1.0 - VISCOSITY_POWER) * logt)
    skew = 1.0 / (15.0 * density * temper * temper)
    cell_ref[0] = ux
    cell_ref[1] = uy
    cell_ref[2] = uz
    cell_ref[3] = 0.5 / temper
    cell_ref[4] = rate * density * jnp.exp(-1.5 * logt)
    cell_ref[5] = extras[1][5] * skew
    cell_ref[6] = extras[1][6] * skew
    cell_ref[7] = extras[1][7] * skew
    cell_ref[8] = 1.0 - rate


def macro_solve(owner_map, own, other, cross):
    vmem = pl.BlockSpec(memory_space=pltpu.VMEM)
    smem = pl.BlockSpec(memory_space=pltpu.SMEM)
    return pl.pallas_call(
        macro_kernel,
        in_specs=[smem] + [vmem] * 3,
        out_specs=[vmem] * 3 + [smem],
        out_shape=[jax.ShapeDtypeStruct((5, SUB, LANES), jnp.float32), jax.ShapeDtypeStruct((9, SUB, LANES), jnp.float32),
                   jax.ShapeDtypeStruct((5, LANES), jnp.float32), jax.ShapeDtypeStruct((1,), jnp.int32)],
        compiler_params=pltpu.CompilerParams(vmem_limit_bytes=SMALL_LIMIT),
        name="macro",
    )(owner_map, own, other, cross)


def kinetic_kernel(bm_ref, scal_ref, drift_ref, mask_ref, cell_ref, f_hbm, out_ref, *refs):
    gz_ref, az_ref, sz_ref, iz_ref, turn_ref, ylow_ref, yhigh_ref, zlow_ref, zhigh_ref, in_sem = refs
    ysides, zsides = (ylow_ref, yhigh_ref), (zlow_ref, zhigh_ref)
    blocks = bm_ref.shape[0]
    half_id = PARTS * NVX // 2
    index = lax.axis_index("space")
    count = lax.axis_size("space")

    def fetch(i):
        return pltpu.make_async_copy(f_hbm.at[pl.ds(i * VB, VB)], out_ref.at[pl.ds(i * VB, VB)], in_sem.at[i])

    for i in range(blocks):
        fetch(i).start()
    plane, spot, along_z = places()
    fixed = mask_ref[...] == 1
    source = lax.broadcasted_iota(jnp.int32, (2 * LANES, LANES), 0) % LANES
    target = lax.broadcasted_iota(jnp.int32, (2 * LANES, LANES), 1)
    for step in (1, 2):
        for sign in (0, 1):
            away = step if sign else -step
            wanted_y = (target + (away * NZ + LANES)) % LANES
            wanted_z = target - target % NZ + (target % NZ + (away + NZ)) % NZ
            for which, wanted in ((sign, wanted_y), (2 + sign, wanted_z)):
                turn_ref[which, :, pl.ds((step - 1) * LANES, LANES)] = jnp.where(source == wanted, 1.0, 0.0).astype(jnp.bfloat16)
    ux, uy, uz, inv2t = cell_ref[0], cell_ref[1], cell_ref[2], cell_ref[3]
    hot = jnp.full((SUB, LANES), scal_ref[1], jnp.float32)
    hot_inv = 0.5 / hot
    hot_scale = scal_ref[0] * jnp.exp(-1.5 * jnp.log(hot))
    for e in range(NVZ):
        cz = speed(e, DZ)
        rel = cz - uz
        t = rel * rel * inv2t
        gz_ref[e] = jnp.exp(-t)
        sz_ref[e] = 2.0 * t
        az_ref[e] = rel * cell_ref[7]
        off = cz - drift_ref[2]
        iz_ref[e] = jnp.exp(-(off * off) * hot_inv)

    part_rows = ROWS // 2
    part_size = part_rows * NVZ

    def shifts(i, part):
        x = out_ref[pl.ds(i * VB + part * part_size, part_size)].reshape(part_size * SUB, LANES)
        hi = x.astype(jnp.bfloat16)
        lo = (x - hi.astype(jnp.float32)).astype(jnp.bfloat16)
        both = jnp.concatenate([hi, lo], axis=1)
        which = jnp.where((bm_ref[i] % PARTS) >= PARTS // 2, 0, 1)
        ysides[part][...] = jnp.dot(both, turn_ref[which], preferred_element_type=jnp.float32)
        both = both.reshape(part_rows, 2, NVZ * SUB // 2, 2 * LANES)
        for side in (0, 1):
            lines = both[:, side].reshape(part_size * SUB // 2, 2 * LANES)
            zsides[part][side] = jnp.dot(lines, turn_ref[3 - side], preferred_element_type=jnp.float32)

    fetch(0).wait()
    shifts(0, 0)

    def run(i, carry):
        block = bm_ref[i]
        positive = block >= half_id
        y_positive = (block % PARTS) >= PARTS // 2
        cx, cy0 = block_speeds(block)

        @pl.when(i + 1 < blocks)
        def _():
            fetch(i + 1).wait()
        following = jnp.minimum(i + 1, blocks - 1)
        k0x, k1x, k2x = upwind(KINETIC_STEP * jnp.abs(cx))
        relx = cx - ux
        tx = relx * relx * inv2t
        ax = relx * cell_ref[5]
        offx = cx - drift_ref[0]

        cross1 = jnp.where(y_positive, spot, LANES - 1 - spot) < NZ
        cross2 = jnp.where(y_positive, spot, LANES - 1 - spot) < 2 * NZ

        def rows(turn, stay_k, near_k, far_k, enter_k):
            def one(y):
                yside_ref, zside_ref = ysides[y // part_rows], zsides[y // part_rows]
                r = y % part_rows
                cy = cy0 + y * DY
                k0y, k1y, k2y = upwind(KINETIC_STEP * jnp.abs(cy))
                rely = cy - uy
                txy = tx + rely * rely * inv2t
                axy = ax + rely * cell_ref[6]
                gxy = cell_ref[4] * jnp.exp(-txy)
                sxy = 2.0 * txy - 5.0
                keep = stay_k - k0y
                offy = cy - drift_ref[1]
                ixy = hot_scale * jnp.exp(-(offx * offx + offy * offy) * hot_inv)
                for e in range(NVZ):
                    k0z, k1z, k2z = upwind(KINETIC_STEP * abs(speed(e, DZ)))
                    spot_v = i * VB + y * NVZ + e
                    f = out_ref[spot_v]
                    inflow = ixy * iz_ref[e]
                    total = f * (keep - k0z)
                    total = total - near_k * sublane(turn)(f) - far_k * sublane(2 * turn)(f)
                    if turn > 0:
                        total = total - enter_k * inflow
                    lines = pl.ds((r * NVZ + e) * SUB, SUB)
                    y1 = yside_ref[lines, :LANES]
                    y2 = yside_ref[lines, LANES:]
                    lines = pl.ds((r * (NVZ // 2) + e % (NVZ // 2)) * SUB, SUB)
                    z1 = zside_ref[e // (NVZ // 2), lines, :LANES]
                    z2 = zside_ref[e // (NVZ // 2), lines, LANES:]
                    y1 = jnp.where(cross1, sublane(4)(y1), y1)
                    y2 = jnp.where(cross2, sublane(4)(y2), y2)
                    total = total - k1y * y1 - k2y * y2
                    total = total - k1z * z1 - k2z * z2
                    shape = 1.0 + (axy + az_ref[e]) * (sxy + sz_ref[e])
                    total = total + (gxy * gz_ref[e]) * shape
                    out_ref[spot_v] = jnp.where(fixed, inflow, total)

            shifts(i, 1)
            for y in range(part_rows):
                one(y)
            shifts(following, 0)
            for y in range(part_rows, ROWS):
                one(y)

        @pl.when(positive)
        def _():
            near_k = jnp.where(plane == 0, 0.0, k1x)
            far_k = jnp.where(plane < 2, 0.0, k2x)
            bring = jnp.where(index == 0, 1.0, 0.0)
            enter_k = ((k1x - near_k) + (k2x - far_k)) * bring
            rows(1, cell_ref[8] - k0x, near_k, far_k, enter_k)

        @pl.when(jnp.logical_not(positive))
        def _():
            last = jnp.where(index == count - 1, 1.0, 0.0)
            near_k = jnp.where(plane == 3, 0.0, k1x) + jnp.where(plane == 2, k2x, 0.0) * last
            far_k = jnp.where(plane >= 2, 0.0, k2x)
            stay_k = cell_ref[8] - k0x - jnp.where(plane == 3, k1x + k2x, 0.0) * last
            rows(-1, stay_k, near_k, far_k, None)

        return carry

    lax.fori_loop(0, blocks, run, 0)


def kinetic(f, block_map, scalars, drift, mask, cells):
    blocks = block_map.shape[0]
    smem = pl.BlockSpec(memory_space=pltpu.SMEM)
    vmem = pl.BlockSpec(memory_space=pltpu.VMEM)
    table = pltpu.VMEM((NVZ, SUB, LANES), jnp.float32)
    yside = pltpu.VMEM((VB * SUB // 2, 2 * LANES), jnp.float32)
    zside = pltpu.VMEM((2, VB * SUB // 4, 2 * LANES), jnp.float32)
    return pl.pallas_call(
        kinetic_kernel,
        in_specs=[smem, smem, smem, vmem, vmem, pl.BlockSpec(memory_space=pltpu.HBM)],
        out_specs=vmem,
        out_shape=pltpu.VMEM(f.shape, jnp.float32),
        scratch_shapes=[table, table, table, table, pltpu.VMEM((4, 2 * LANES, 2 * LANES), jnp.bfloat16),
                        yside, yside, zside, zside, pltpu.SemaphoreType.DMA((blocks,))],
        compiler_params=pltpu.CompilerParams(vmem_limit_bytes=KINETIC_LIMIT),
        name="kinetic",
    )(block_map, scalars, drift, mask, cells, in_hbm(f))


def halo_kernel(sizes, bm_ref, mask_ref, part_ref, *refs):
    kinds = sum(1 for size in sizes if size)
    up = refs[:kinds]
    down = refs[kinds:2 * kinds]
    out_hbm, obuf, late, out_sem, late_sem = refs[2 * kinds:]
    blocks = bm_ref.shape[0]
    half_id = PARTS * NVX // 2
    half = VB // 2
    index = lax.axis_index("space")
    count = lax.axis_size("space")
    plane, _, _ = places()
    fixed = mask_ref[...] == 1

    def run(i, positives):
        block = bm_ref[i]
        positive = block >= half_id
        rank = jnp.where(positive, positives, i - positives)
        cx, _ = block_speeds(block)
        _, k1x, k2x = upwind(KINETIC_STEP * jnp.abs(cx))
        outer = jnp.where(positive, index == 0, index == count - 1)

        def rows(x_up, source, base):
            if x_up:
                near, far = plane == 3, plane >= 2
            else:
                near, far = plane == 0, plane < 2
            turn = 1 if x_up else -1

            def body(y, carry):
                for e in range(NVZ // 2):
                    pair = source[base + y * (NVZ // 2) + e]
                    for side in (0, 1):
                        halo = sublane(2 * turn)(pair) if side else pair
                        spot_v = i * VB + y * NVZ + e + side * (NVZ // 2)
                        brought = sublane(turn)(jnp.where(near, halo * k1x, 0.0)) + sublane(2 * turn)(jnp.where(far, halo * k2x, 0.0))
                        old = part_ref[spot_v]
                        obuf[spot_v] = jnp.where(fixed, old, old - brought)
                return carry

            lax.fori_loop(0, ROWS, body, 0)

        @pl.when(outer)
        def _():
            def body(y, carry):
                for e in range(NVZ):
                    obuf[i * VB + y * NVZ + e] = part_ref[i * VB + y * NVZ + e]
                return carry

            lax.fori_loop(0, ROWS, body, 0)

        inner = jnp.logical_not(outer)
        for x_up in (True, False):
            mine = jnp.logical_and(inner, positive if x_up else jnp.logical_not(positive))
            source = up if x_up else down

            @pl.when(jnp.logical_and(mine, rank < sizes[0]))
            def _(x_up=x_up, source=source):
                rows(x_up, source[0], rank * half)

            if kinds > 1:
                @pl.when(jnp.logical_and(mine, rank >= sizes[0]))
                def _(x_up=x_up, source=source):
                    copy = pltpu.make_async_copy(source[1].at[pl.ds((rank - sizes[0]) * half, half)], late, late_sem)
                    copy.start()
                    copy.wait()
                    rows(x_up, late, 0)
        pltpu.make_async_copy(obuf.at[pl.ds(i * VB, VB)], out_hbm.at[pl.ds(i * VB, VB)], out_sem.at[i]).start()
        return positives + jnp.where(positive, 1, 0)

    lax.fori_loop(0, blocks, run, jnp.int32(0))

    def drain(i, carry):
        pltpu.make_async_copy(obuf.at[pl.ds(i * VB, VB)], out_hbm.at[pl.ds(i * VB, VB)], out_sem.at[i]).wait()
        return carry

    lax.fori_loop(0, blocks, drain, 0)


def halo_update(part, block_map, mask, sizes, up, down):
    blocks = block_map.shape[0]
    smem = pl.BlockSpec(memory_space=pltpu.SMEM)
    vmem = pl.BlockSpec(memory_space=pltpu.VMEM)
    hbm = pl.BlockSpec(memory_space=pltpu.HBM)
    places_of = ([vmem] + [hbm] * (len(up) - 1)) * 2
    return pl.pallas_call(
        functools.partial(halo_kernel, sizes),
        in_specs=[smem, vmem, vmem] + places_of,
        out_specs=hbm,
        out_shape=jax.ShapeDtypeStruct(part.shape, jnp.float32),
        scratch_shapes=[pltpu.VMEM((blocks * VB, SUB, LANES), jnp.float32), pltpu.VMEM((VB // 2, SUB, LANES), jnp.float32),
                        pltpu.SemaphoreType.DMA((blocks,)), pltpu.SemaphoreType.DMA],
        compiler_params=pltpu.CompilerParams(vmem_limit_bytes=KINETIC_LIMIT),
        name="halo",
    )(block_map, mask, part, in_vmem(up[0]), *map(in_hbm, up[1:]), in_vmem(down[0]), *map(in_hbm, down[1:]))


def over_vel(values):
    count = lax.axis_size("vel")
    if count & (count - 1):
        return lax.psum(values, "vel")
    reach = 1
    while reach < count:
        values = values + lax.ppermute(values, "vel", [(i, i ^ reach) for i in range(count)])
        reach *= 2
    return values


def tiles(array):
    lead, planes, width = array.shape
    return array.reshape(lead, planes, width // LANES, LANES).transpose(0, 2, 1, 3).reshape(lead, planes * width // LANES, LANES)


def per_device(distribution, block_map, inflow_mask, owner_map, inflow_scalars, inflow_drift):
    vel_count = lax.axis_size("vel")
    vel_index = lax.axis_index("vel")
    space_count = lax.axis_size("space")
    local_vel, planes, width = distribution.shape
    assert planes == MSTEPS and planes * width == SUB * LANES
    block_len = planes * width // vel_count
    blocks = block_map.shape[0]
    sizes = slot_sizes(blocks)
    f = tiles(distribution)
    mask = tiles(inflow_mask[None])[0]
    rise = [(i, i + 1) for i in range(space_count - 1)]
    fall = [(i + 1, i) for i in range(space_count - 1)]

    partial, ups, downs = gather(f, block_map, sizes)
    got_up = [lax.ppermute(ups[0], "space", rise)]
    got_down = [lax.ppermute(downs[0], "space", fall)]
    total = over_vel(partial)
    other = lax.ppermute(total, "space", [(i, i ^ 1) for i in range(space_count)])
    cross = lax.ppermute(other, "space", [(i, i + 2) for i in range(0, space_count - 2, 2)]
                         + [(i, i - 2) for i in range(3, space_count, 2)])
    macro, cells, mine, flag = macro_solve(owner_map, total, other, cross)
    part = kinetic(f, block_map, inflow_scalars, inflow_drift, mask, cells)
    if sizes[1]:
        extra = lax.cond(flag[0] > 0,
                         lambda a, b: (lax.ppermute(a, "space", rise), lax.ppermute(b, "space", fall)),
                         lambda a, b: (a, b), ups[1], downs[1])
        got_up.append(extra[0])
        got_down.append(extra[1])
    updated = halo_update(part, block_map, mask, sizes, got_up, got_down)
    current = updated.reshape(local_vel, width // LANES, planes, LANES).transpose(0, 2, 1, 3).reshape(local_vel, planes, width)
    if block_len != LANES:
        flat = macro.reshape(5, width // LANES, planes, LANES).transpose(0, 2, 1, 3).reshape(5, vel_count, block_len)
        mine = lax.dynamic_slice_in_dim(flat, owner_map[vel_index], 1, axis=1).reshape(5, block_len)
    return (current, mine)


def solution(mesh):
    return jax.shard_map(
        per_device,
        mesh=mesh,
        in_specs=(P("vel", "space", None), P("vel"), P("space", None), P(), P(), P()),
        out_specs=(P("vel", "space", None), P(None, ("space", "vel"))),
        check_vma=False,
    )
```
